32 devices in a mesh: tm: 4 (over x, core), space: 8 (over z, y).
Axes of the slice: x: 2, y: 2, z: 4, core: 2. Of those that a mesh axis runs over, the one named last changes fastest.
Arguments:
- initial_state: float32 [512, 3, 512], P('space'), may hold values from -1 to 1, as said below
- applied_field: float32 [512, 3, 512], P('space'), may hold values from -2 to 2
- coupling: float32 [512, 512], P('space'), may hold values from 0.5 to 2
Outputs:
- slice_states: float32 [4, 512, 3, 512], P('tm', 'space')
The draws below stay inside these ranges and needn't reach their ends.
Inputs may be any that keep to these rules, and one draw needn't show every extreme that they name: `initial_state`: every cell's three components form a vector of length one.
All inputs are finite; a program needn't handle non-finite values.
Results may differ from the reference program's by a relative error of at most 0.00014.
Values sent between devices are 32-bit elements; how exact they have to be, the bound alone decides.
A program may use at most 128 MiB of HBM per device.

```python
import math
import jax
import jax.numpy as jnp

GRID = 512
FINE = 2
ITERS = 1
SLICES = 4


def base_frame(key):
    frame_key = jax.random.fold_in(key, 7)
    sign_key, tilt_key = jax.random.split(frame_key)
    signs = (2 * jax.random.randint(sign_key, (3,), 0, 2) - 1).astype(jnp.float32)
    tilt = jax.random.uniform(tilt_key, (), jnp.float32, 0.6, 0.9)
    return (signs, tilt)


def draw_initial_state(key, part):
    signs, tilt = base_frame(key)
    noise_key = jax.random.fold_in(key, 11)
    in_plane = jnp.cos(tilt) / math.sqrt(2.0)
    base = jnp.stack([signs[0] * in_plane, signs[1] * in_plane, signs[2] * jnp.sin(tilt)]).reshape(1, 3, 1)
    noise = jax.random.uniform(noise_key, (GRID, 3, GRID), jnp.float32, -0.45, 0.45)
    vector = base + noise
    length = jnp.sqrt(jnp.sum(vector * vector, axis=1, keepdims=True))
    return vector / length


def draw_applied_field(key, part):
    signs, tilt = base_frame(key)
    noise_key = jax.random.fold_in(key, 13)
    field_scale = 2.5 / math.sqrt(2.0)
    base = jnp.stack([-signs[1] * field_scale, signs[0] * field_scale, 0.0 * field_scale]).reshape(1, 3, 1)
    noise = 0.4 * jax.random.normal(noise_key, (GRID, 3, GRID), jnp.float32)
    return jnp.clip(base + noise, -2.0, 2.0)


def shard_levels(rng, dims, cuts, low, top_value):
    def one(dim, blocks):
        steps = jax.random.uniform(jax.random.fold_in(jax.random.fold_in(rng, 6), dim), (blocks,), jnp.float32, low / len(cuts), top_value / len(cuts))
        return jnp.repeat(jnp.exp(steps), dims[dim] // blocks).reshape((-1,) + (1,) * (len(dims) - dim - 1))

    gain = one(*cuts[0])
    for cut in cuts[1:]:
        gain = gain * one(*cut)
    return gain


def setup_inputs(seed: int = 0) -> dict:
    arg_keys = jax.random.split(jax.random.key(seed), 4)
    initial_state = draw_initial_state(jax.random.fold_in(arg_keys[3], 71), 0)
    applied_field = draw_applied_field(jax.random.fold_in(arg_keys[3], 71), 0)
    coupling = jnp.clip(jnp.exp(math.log(2.0) - 1.3862944 * jax.random.uniform(arg_keys[2], (GRID, GRID), jnp.float32) ** shard_levels(arg_keys[2], (GRID, GRID), ((0, 8),), -0.2, 0.2)), 0.5, 2.0)
    return dict(initial_state=initial_state, applied_field=applied_field, coupling=coupling)


step_time = 0.06
damping = 0.02
stiffness = 0.25
thickness = 8.0

def spectral_tensor(row_index, column_index, length):
    half_length = length // 2
    signed_rows = jnp.where(row_index < half_length, row_index, row_index - length).astype(jnp.float32)
    signed_columns = jnp.where(column_index < half_length, column_index, column_index - length).astype(jnp.float32)
    wave_rows = 2.0 * math.pi / length * signed_rows[:, None]
    wave_columns = 2.0 * math.pi / length * signed_columns[None, :]
    squared = wave_rows * wave_rows + wave_columns * wave_columns
    nonzero = squared > 0.0
    safe_square = jnp.where(nonzero, squared, 1.0)
    scaled_wave = jnp.sqrt(safe_square) * thickness
    film_factor = jnp.where(nonzero, (1.0 - jnp.exp(-scaled_wave)) / scaled_wave, 1.0)
    in_plane = (1.0 - film_factor) / safe_square
    nyquist = (row_index[:, None] == half_length) | (column_index[None, :] == half_length)
    normalizer = -1.0 / (length * length)
    tensor_first = in_plane * wave_columns * wave_columns * normalizer
    tensor_second = in_plane * wave_rows * wave_rows * normalizer
    tensor_cross = jnp.where(nyquist, 0.0, in_plane * wave_columns * wave_rows) * normalizer
    tensor_normal = film_factor * normalizer
    return (tensor_first, tensor_second, tensor_cross, tensor_normal)

def exchange_field(padded_state, padded_coupling):
    center_state = padded_state[1:-1]
    center_coupling = padded_coupling[1:-1]
    wide_state = jnp.pad(padded_state, ((0, 0), (0, 0), (1, 1)))
    wide_coupling = jnp.pad(padded_coupling, ((0, 0), (1, 1)))
    neighbour_sum = padded_coupling[2:, None, :] * (padded_state[2:] - center_state)
    neighbour_sum = neighbour_sum + padded_coupling[:-2, None, :] * (padded_state[:-2] - center_state)
    neighbour_sum = neighbour_sum + wide_coupling[1:-1, None, 2:] * (wide_state[1:-1, :, 2:] - center_state)
    neighbour_sum = neighbour_sum + wide_coupling[1:-1, None, :-2] * (wide_state[1:-1, :, :-2] - center_state)
    return stiffness * center_coupling[:, None, :] * neighbour_sum

def torque(magnet, effective):
    first_cross = jnp.cross(magnet, effective, axis=1)
    second_cross = jnp.cross(magnet, first_cross, axis=1)
    return -(first_cross + damping * second_cross) / (1.0 + damping * damping)

def demag_field(magnet):
    padded = jnp.pad(magnet, ((0, GRID), (0, 0), (0, GRID)))
    spectrum = jnp.fft.fft2(padded, axes=(0, 2))
    index_all = jnp.arange(2 * GRID, dtype=jnp.int32)
    tensor_first, tensor_second, tensor_cross, tensor_normal = spectral_tensor(index_all, index_all, 2 * GRID)
    first_out = tensor_first * spectrum[:, 0] + tensor_cross * spectrum[:, 1]
    second_out = tensor_cross * spectrum[:, 0] + tensor_second * spectrum[:, 1]
    third_out = tensor_normal * spectrum[:, 2]
    combined = jnp.stack([first_out, second_out, third_out], axis=1)
    result = jnp.fft.ifft2(combined, axes=(0, 2)) * float(2 * GRID * (2 * GRID))
    return jnp.real(result)[:GRID, :, :GRID].astype(jnp.float32)

def effective_fine(magnet, applied_field, padded_coupling):
    padded_state = jnp.pad(magnet, ((1, 1), (0, 0), (0, 0)))
    return exchange_field(padded_state, padded_coupling) + demag_field(magnet) + applied_field

def propagate_fine(magnet, applied_field, padded_coupling):
    for repeat in range(FINE):
        first_rate = torque(magnet, effective_fine(magnet, applied_field, padded_coupling))
        predicted = magnet + step_time * first_rate
        second_rate = torque(predicted, effective_fine(predicted, applied_field, padded_coupling))
        magnet = magnet + 0.5 * step_time * (first_rate + second_rate)
    return magnet

def propagate_coarse(magnet, applied_field, padded_coupling):
    padded_state = jnp.pad(magnet, ((1, 1), (0, 0), (0, 0)))
    local_demag = jnp.array([0.0, 0.0, -1.0], dtype=jnp.float32).reshape(1, 3, 1)
    effective = exchange_field(padded_state, padded_coupling) + applied_field + magnet * local_demag
    return magnet + FINE * step_time * torque(magnet, effective)

def coarse_sweep(differences, initial_state, applied_field, padded_coupling):
    current = initial_state
    starts = []
    coarse_ends = []
    slice_ends = []
    for slice_number in range(SLICES):
        predicted = propagate_coarse(current, applied_field, padded_coupling)
        advanced = predicted + differences[slice_number]
        starts.append(current)
        coarse_ends.append(predicted)
        slice_ends.append(advanced)
        current = advanced
    return (starts, coarse_ends, slice_ends)

def reference(initial_state, applied_field, coupling):
    padded_coupling = jnp.pad(coupling, ((1, 1), (0, 0)))
    differences = [jnp.zeros_like(initial_state) for slice_number in range(SLICES)]
    starts, coarse_ends, slice_ends = coarse_sweep(differences, initial_state, applied_field, padded_coupling)
    for iteration in range(ITERS):
        differences = [propagate_fine(starts[slice_number], applied_field, padded_coupling) - coarse_ends[slice_number] for slice_number in range(SLICES)]
        starts, coarse_ends, slice_ends = coarse_sweep(differences, initial_state, applied_field, padded_coupling)
    return jnp.stack(slice_ends, axis=0)
```

```python
import functools
import math

import jax
import jax.numpy as jnp
import numpy as np
from jax import lax
from jax.experimental import pallas as pl
from jax.experimental.pallas import tpu as pltpu
from jax.sharding import Mesh, PartitionSpec as P

FINE = 2
step_time = 0.06
damping = 0.02
stiffness = 0.25
thickness = 8.0
PASSES = 3

EVERY = ("x", "core", "zh", "rest")


def sector_tables(grid):
    half = grid // 2
    place = 2 * np.arange(half) - (grid - 1)
    wave = np.arange(grid)
    odd_wave = np.where(wave == 0, grid, wave)
    turn = 4 * grid

    def angle(k):
        return 2.0 * np.pi / turn * ((place[:, None] * k[None, :]) % turn)

    table = np.stack([np.cos(angle(wave)), np.sin(angle(odd_wave))]).astype(np.float32)
    fold = np.zeros((grid, grid), np.float32)
    for i in range(half):
        fold[i, i] = fold[grid - 1 - i, i] = fold[i, half + i] = 1.0
        fold[grid - 1 - i, half + i] = -1.0
    return table, fold


def exchange_field(padded, pad_coupling):
    center = padded[:, 1:-1]
    coupling = pad_coupling[1:-1]
    wide = jnp.pad(padded[:, 1:-1], ((0, 0), (0, 0), (1, 1)))
    wide_coupling = jnp.pad(coupling, ((0, 0), (1, 1)))
    total = pad_coupling[2:] * (padded[:, 2:] - center)
    total = total + pad_coupling[:-2] * (padded[:, :-2] - center)
    total = total + wide_coupling[:, 2:] * (wide[:, :, 2:] - center)
    total = total + wide_coupling[:, :-2] * (wide[:, :, :-2] - center)
    return stiffness * coupling * total


def cross(a, b):
    return jnp.stack([a[1] * b[2] - a[2] * b[1], a[2] * b[0] - a[0] * b[2], a[0] * b[1] - a[1] * b[0]])


def torque(magnet, effective):
    first = cross(magnet, effective)
    return -(first + damping * cross(magnet, first)) * (1.0 / (1.0 + damping * damping))


def coarse(padded, pad_coupling, field):
    center = padded[:, 1:-1]
    effective = exchange_field(padded, pad_coupling) + field
    effective = jnp.stack([effective[0], effective[1], effective[2] - center[2]])
    return center + FINE * step_time * torque(center, effective)


def halves(table):
    high = table.astype(jnp.bfloat16)
    return [high, (table - high.astype(np.float32)).astype(jnp.bfloat16)]


def split(value):
    high = value.astype(jnp.bfloat16)
    return high, (value - high.astype(jnp.float32)).astype(jnp.bfloat16)


def dot3(left_high, left_low, right_high, right_low):
    def one(a, b):
        return jnp.dot(a, b, preferred_element_type=jnp.float32)

    return one(left_high, right_high) + (one(left_high, right_low) + one(left_low, right_high))


def cross_of(a, b):
    return [a[1] * b[2] - a[2] * b[1], a[2] * b[0] - a[0] * b[2], a[0] * b[1] - a[1] * b[0]]


def product(passes, left, right):
    def one(a, b):
        return jnp.dot(a, b, preferred_element_type=jnp.float32)

    value = one(left[0], right[0])
    if passes > 1:
        value = value + one(left[1], right[0])
    if passes > 2:
        value = value + one(left[0], right[1])
    return value


def put(passes, pair, where, value):
    high, low = split(value)
    pair[0][where] = high
    if passes > 1:
        pair[1][where] = low


def fine_kernel(
    space,
    mine, theirs, field, coupling,
    table_high, table_low, turned_high, turned_low, fold, unfold,
    out,
    current, rate, base, probe, demag, far_start, far_field, far_coupling, links, tensors,
    edge_out, edge_in, wide_high, wide_low, send_xy, send_z, land, back, got_xy, got_z,
    plane_high, plane_low, mixed_high, mixed_low,
    swap_sems, edge_sems, send_sems, land_sems, back_sems, got_sems,
):
    _, strip, grid = mine.shape
    rest_count = space // 2
    half = grid // 2
    multi = rest_count // 4
    width = grid // multi
    core, zh, rest = lax.axis_index("core"), lax.axis_index("zh"), lax.axis_index("rest")
    order = jnp.where(zh == 0, rest, rest_count - 1 - rest)
    number = 2 * order + core
    unit = rest // multi
    share = rest % multi
    row_odd, column_odd = unit // 2, unit % 2

    def at_place(core_index, rest_index):
        return {"core": core_index, "rest": rest_index}

    def owner(index):
        place = index // 2
        return at_place(index % 2, jnp.where(zh == 0, place, rest_count - 1 - place))

    def remote(source, target, send_sem, recv_sem, where):
        return pltpu.make_async_remote_copy(
            src_ref=source, dst_ref=target, send_sem=send_sem, recv_sem=recv_sem,
            device_id=where, device_id_type=pl.DeviceIdType.MESH,
        )

    barrier = pltpu.get_barrier_semaphore()
    partner = {"zh": 1 - zh, "rest": rest_count - 1 - rest}

    def greet(k, carry):
        pl.semaphore_signal(
            barrier, inc=1, device_id=owner((number + k) % space), device_id_type=pl.DeviceIdType.MESH
        )
        return carry

    lax.fori_loop(1, space, greet, 0)
    pl.semaphore_signal(barrier, inc=1, device_id=partner, device_id_type=pl.DeviceIdType.MESH)
    pl.semaphore_wait(barrier, space)

    swaps = [
        remote(source, target, swap_sems.at[0, n], swap_sems.at[1, n], partner)
        for n, (source, target) in enumerate(
            ((theirs, far_start), (field, far_field), (coupling, far_coupling))
        )
    ]
    for swap in swaps:
        swap.start()

    def fill(i, carry):
        at = pl.multiple_of(i * 64, 64)
        slot_rows = at + lax.broadcasted_iota(jnp.int32, (64, width), 0)
        slot_columns = share * width + lax.broadcasted_iota(jnp.int32, (64, width), 1)
        unit_length = 2.0 * math.pi / (2 * grid)

        def parts(odd_rows, odd_columns):
            rows = jnp.where((slot_rows == 0) & (odd_rows == 1), grid, slot_rows)
            columns = jnp.where((slot_columns == 0) & (odd_columns == 1), grid, slot_columns)
            wave_rows = unit_length * rows.astype(jnp.float32)
            wave_columns = unit_length * columns.astype(jnp.float32)
            squared = wave_rows * wave_rows + wave_columns * wave_columns
            nonzero = squared > 0.0
            safe = jnp.where(nonzero, squared, 1.0)
            scaled = jnp.sqrt(safe) * thickness
            film = jnp.where(nonzero, (1.0 - jnp.exp(-scaled)) / scaled, 1.0)
            weight = jnp.where(slot_rows == 0, 1.0, 2.0) * jnp.where(slot_columns == 0, 1.0, 2.0)
            weight = weight * (-1.0 / (4 * grid * grid))
            return wave_rows, wave_columns, film, (1.0 - film) / safe, weight

        @pl.when(core == 1)
        def _():
            wave_rows, wave_columns, _, in_plane, weight = parts(row_odd, column_odd)
            tensors[0, pl.ds(at, 64), :] = in_plane * wave_columns * wave_columns * weight
            mixed = in_plane * wave_columns * wave_rows * weight
            sign = jnp.where((row_odd == column_odd) == (zh == 0), -1.0, 1.0)
            tensors[2, pl.ds(at, 64), :] = jnp.where((slot_rows == 0) | (slot_columns == 0), 0.0, mixed * sign)
            wave_rows, wave_columns, _, in_plane, weight = parts(1 - row_odd, 1 - column_odd)
            tensors[1, pl.ds(at, 64), :] = in_plane * wave_rows * wave_rows * weight

        @pl.when(core == 0)
        def _():
            _, _, film, _, weight = parts(row_odd, column_odd)
            tensors[0, pl.ds(at, 64), :] = film * weight

        return carry

    lax.fori_loop(0, grid // 64, fill, 0)

    def make_links(t, source):
        own = source[8 : 8 + strip, :]
        lane = lax.broadcasted_iota(jnp.int32, (strip, grid), 1)
        links[t, 0] = stiffness * own * source[7 : 7 + strip, :]
        links[t, 1] = stiffness * own * source[9 : 9 + strip, :]
        links[t, 2] = jnp.where(lane == 0, 0.0, stiffness * own * pltpu.roll(own, 1, 1))
        links[t, 3] = jnp.where(lane == grid - 1, 0.0, stiffness * own * pltpu.roll(own, grid - 1, 1))

    make_links(0, coupling)
    base[0] = mine[...]
    swaps[0].wait()
    base[1] = far_start[...]
    current[:, :, 8 : 8 + strip, :] = base[...]
    probe[...] = base[...]

    def to_unit(kind, r):
        target = (rest + r) % rest_count
        if kind == 1:
            source, landing = send_xy.at[target // multi], land.at[:, pl.ds(number * strip, strip), :]
        else:
            source, landing = send_z.at[target // multi], land.at[0, pl.ds(number * strip, strip), :]
        return remote(source, landing, send_sems.at[kind, r], land_sems.at[number], at_place(kind, target))

    def landed(kind, index):
        if kind == 1:
            source, landing = send_xy.at[0], land.at[:, pl.ds(index * strip, strip), :]
        else:
            source, landing = send_z.at[0], land.at[0, pl.ds(index * strip, strip), :]
        return remote(source, landing, send_sems.at[kind, 0], land_sems.at[index], owner(index))

    def to_owner(kind, k):
        index = (number + k) % space
        if kind == 1:
            source, landing = back.at[:, pl.ds(index * strip, strip), :], got_xy.at[rest]
        else:
            source, landing = back.at[0, pl.ds(index * strip, strip), :], got_z.at[rest]
        return remote(source, landing, back_sems.at[k], got_sems.at[kind, rest], owner(index))

    def gotten(kind, r):
        if kind == 1:
            source, landing = back.at[:, pl.ds(0, strip), :], got_xy.at[r]
        else:
            source, landing = back.at[0, pl.ds(0, strip), :], got_z.at[r]
        return remote(source, landing, back_sems.at[0], got_sems.at[kind, r], at_place(kind, r))

    def transform(kind, passes):
        planes = [(row_odd, column_odd), (1 - row_odd, 1 - column_odd)] if kind == 1 else [(row_odd, column_odd)]
        columns = pl.ds(pl.multiple_of(share * width, width), width)
        for n, (_, odd) in enumerate(planes):
            spectrum = product(
                passes, split(land[n]), (table_high[odd, :, columns], table_low[odd, :, columns])
            )
            put(passes, (plane_high, plane_low), n, spectrum)
        step = half

        def mix(i, carry):
            at = pl.multiple_of(i * step, step)
            lines = pl.ds(at, step)
            both = [
                product(
                    passes, (turned_high[odd, lines, :], turned_low[odd, lines, :]), (plane_high[n], plane_low[n])
                )
                for n, (odd, _) in enumerate(planes)
            ]
            if kind == 1:
                cross_term = tensors[2, lines, :]
                values = [
                    tensors[0, lines, :] * both[0] + cross_term * both[1],
                    cross_term * both[0] + tensors[1, lines, :] * both[1],
                ]
            else:
                values = [tensors[0, lines, :] * both[0]]
            for n, value in enumerate(values):
                put(passes, (mixed_high, mixed_low), (n, lines), value)
            return carry

        lax.fori_loop(0, grid // step, mix, 0)
        for n, (odd_rows, odd_columns) in enumerate(planes):
            film = product(
                passes, (table_high[odd_rows], table_low[odd_rows]), (mixed_high[n], mixed_low[n])
            )
            back[n] = product(
                passes, split(film), (turned_high[odd_columns, columns, :], turned_low[odd_columns, columns, :])
            )

    def unit_work(kind, passes):
        @pl.when(core == kind)
        def _():
            def take(k, carry):
                landed(kind, (number + k) % space).wait_recv()
                return carry

            lax.fori_loop(1, space, take, 0)
            transform(kind, passes)

            def push(k, carry):
                to_owner(kind, k).start()
                return carry

            lax.fori_loop(1, space, push, 0)
            own = pl.ds(pl.multiple_of(number * strip, strip), strip)
            if kind == 1:
                got_xy[rest] = back[:, own, :]
            else:
                got_z[rest] = back[0, own, :]

    def unit_end(kind):
        @pl.when(core == kind)
        def _():
            def drain(k, carry):
                to_owner(kind, k).wait_send()
                return carry

            lax.fori_loop(1, space, drain, 0)

    def evaluate(parity, passes, first):
        for t in range(2):
            for c in range(3):
                edge_out[0, 3 * t + c : 3 * t + c + 1, :] = current[t, c, 8:9, :]
                edge_out[1, 3 * t + c : 3 * t + c + 1, :] = current[t, c, 7 + strip : 8 + strip, :]
        outward = remote(
            edge_out.at[0], edge_in.at[parity, 1], edge_sems.at[parity, 0], edge_sems.at[parity, 1], owner((number + space - 1) % space)
        )
        inward = remote(
            edge_out.at[1], edge_in.at[parity, 0], edge_sems.at[parity, 2], edge_sems.at[parity, 3], owner((number + 1) % space)
        )
        fold_passes = min(passes, 2)
        for c in range(3):
            near, far = probe[0, c], probe[1, c]
            for p, value in enumerate((near + far, near - far)):
                put(fold_passes, (wide_high, wide_low), pl.ds((3 * p + c) * strip, strip), value)
        folded = product(fold_passes, (wide_high[...], wide_low[...]), (fold[...],))
        for p in range(2):
            for q in range(2):
                for c in range(3):
                    piece = folded[(3 * p + c) * strip : (3 * p + c + 1) * strip, q * half : (q + 1) * half]
                    if c == 0:
                        send_xy[2 * p + q, 0] = piece
                    elif c == 1:
                        send_xy[2 * (1 - p) + 1 - q, 1] = piece
                    else:
                        send_z[2 * p + q] = piece

        def launch(r, carry):
            for kind in range(2):
                @pl.when((core != kind) | (r != 0))
                def _(kind=kind):
                    to_unit(kind, r).start()

            return carry

        lax.fori_loop(0, rest_count, launch, 0)
        outward.start()
        inward.start()
        own = pl.ds(pl.multiple_of(number * strip, strip), strip)

        @pl.when(core == 1)
        def _():
            land[:, own, :] = send_xy[unit]

        @pl.when(core == 0)
        def _():
            land[0, own, :] = send_z[unit]

        unit_work(1, passes)
        unit_work(0, passes)

        def settle(r, carry):
            for kind in range(2):
                @pl.when((core != kind) | (r != 0))
                def _(kind=kind):
                    to_unit(kind, r).wait_send()
                    gotten(kind, (rest + r) % rest_count).wait_recv()

            return carry

        lax.fori_loop(0, rest_count, settle, 0)
        outward.wait()
        inward.wait()
        for p in range(2):
            for q in range(2):
                for c in range(3):
                    source = 2 * (1 - p) + 1 - q if c == 1 else 2 * p + q
                    value = None
                    for k in range(multi):
                        piece = got_z[source * multi + k] if c == 2 else got_xy[source * multi + k, c]
                        value = piece if value is None else value + piece
                    where = (pl.ds((3 * p + c) * strip, strip), pl.ds(q * half, half))
                    put(fold_passes, (wide_high, wide_low), where, value)
        unfolded = product(fold_passes, (wide_high[...], wide_low[...]), (unfold[...],))
        for c in range(3):
            even = unfolded[c * strip : (c + 1) * strip]
            odd = unfolded[(3 + c) * strip : (4 + c) * strip]
            for t, value in enumerate((even + odd, even - odd)):
                if first:
                    demag[0, t, c] = value
                    demag[1, t, c] = value
                elif parity == 0:
                    moved = demag[0, t, c] + value
                    demag[0, t, c] = moved
                    demag[1, t, c] = moved
                else:
                    demag[1, t, c] = demag[0, t, c] + value
        if first:
            for swap in swaps[1:]:
                swap.wait()
            make_links(1, far_coupling)
        unit_end(1)
        unit_end(0)
        last = number == space - 1
        for t in range(2):
            for c in range(3):
                current[t, c, 7:8, :] = edge_in[parity, 0, 3 * t + c : 3 * t + c + 1, :]
                facing = current[1 - t, c, 7 + strip : 8 + strip, :]
                arrived = edge_in[parity, 1, 3 * t + c : 3 * t + c + 1, :]
                current[t, c, 8 + strip : 9 + strip, :] = jnp.where(last, facing, arrived)
        for t in range(2):
            applied = (field, far_field)[t]
            for at in range(0, strip, 8):
                rows = slice(at, at + 8)
                inside = [current[t, c, 8 + at : 16 + at, :] for c in range(3)]
                weights = [links[t, n, rows, :] for n in range(4)]
                effective = []
                for c in range(3):
                    m = inside[c]
                    total = weights[0] * (current[t, c, 7 + at : 15 + at, :] - m)
                    total = total + weights[1] * (current[t, c, 9 + at : 17 + at, :] - m)
                    total = total + weights[2] * (pltpu.roll(m, 1, 1) - m)
                    total = total + weights[3] * (pltpu.roll(m, grid - 1, 1) - m)
                    effective.append(total + demag[1, t, c, rows, :] + applied[c, rows, :])
                turned = cross_of(inside, effective)
                again = cross_of(inside, turned)
                for c in range(3):
                    value = -(turned[c] + damping * again[c]) * (1.0 / (1.0 + damping * damping))
                    if parity == 0:
                        rate[t, c, rows, :] = value
                        probe[t, c, rows, :] = step_time * value
                    else:
                        moved = 0.5 * step_time * (rate[t, c, rows, :] + value)
                        probe[t, c, rows, :] = moved
                        base[t, c, rows, :] = base[t, c, rows, :] + moved
        if parity == 0:
            current[:, :, 8 : 8 + strip, :] = base[...] + probe[...]
        else:
            current[:, :, 8 : 8 + strip, :] = base[...]

    evaluate(0, 3, True)

    def fine_step(i, carry):
        evaluate(1, PASSES, False)
        evaluate(0, PASSES, False)
        return carry

    lax.fori_loop(1, FINE, fine_step, 0)
    evaluate(1, PASSES, False)
    out[...] = base[...]


def fine_states(space, mine, theirs, field, coupling, tables):
    _, strip, grid = mine.shape
    half = grid // 2
    rest_count = space // 2
    width = grid * 4 // rest_count
    f32, bf16 = jnp.float32, jnp.bfloat16
    operands = [mine, theirs, field, coupling, *tables]
    return pl.pallas_call(
        functools.partial(fine_kernel, space),
        out_shape=jax.ShapeDtypeStruct((2, 3, strip, grid), f32),
        in_specs=[pl.BlockSpec(memory_space=pltpu.VMEM)] * len(operands),
        out_specs=pl.BlockSpec(memory_space=pltpu.VMEM),
        scratch_shapes=[
            pltpu.VMEM((2, 3, strip + 16, grid), f32),
            pltpu.VMEM((2, 3, strip, grid), f32),
            pltpu.VMEM((2, 3, strip, grid), f32),
            pltpu.VMEM((2, 3, strip, grid), f32),
            pltpu.VMEM((2, 2, 3, strip, grid), f32),
            pltpu.VMEM((3, strip, grid), f32),
            pltpu.VMEM((3, strip, grid), f32),
            pltpu.VMEM((strip + 16, grid), f32),
            pltpu.VMEM((2, 4, strip, grid), f32),
            pltpu.VMEM((3, grid, width), f32),
            pltpu.VMEM((2, 8, grid), f32),
            pltpu.VMEM((2, 2, 8, grid), f32),
            pltpu.VMEM((6 * strip, grid), bf16),
            pltpu.VMEM((6 * strip, grid), bf16),
            pltpu.VMEM((4, 2, strip, half), f32),
            pltpu.VMEM((4, strip, half), f32),
            pltpu.VMEM((2, half, half), f32),
            pltpu.VMEM((2, half, half), f32),
            pltpu.VMEM((rest_count, 2, strip, half), f32),
            pltpu.VMEM((rest_count, strip, half), f32),
            pltpu.VMEM((2, half, width), bf16),
            pltpu.VMEM((2, half, width), bf16),
            pltpu.VMEM((2, grid, width), bf16),
            pltpu.VMEM((2, grid, width), bf16),
            pltpu.SemaphoreType.DMA((2, 3)),
            pltpu.SemaphoreType.DMA((2, 4)),
            pltpu.SemaphoreType.DMA((2, rest_count)),
            pltpu.SemaphoreType.DMA((space,)),
            pltpu.SemaphoreType.DMA((space,)),
            pltpu.SemaphoreType.DMA((2, rest_count)),
        ],
        compiler_params=pltpu.CompilerParams(
            collective_id=0, has_side_effects=True, vmem_limit_bytes=56 * 1024 * 1024
        ),
    )(*operands)


def sweep_kernel(
    space, tm, fine, coarse_end, field, links, out,
    current, landed, edge_out, edge_in, jump_sends, jump_recvs, send_sems, recv_sems,
):
    _, rows, grid = coarse_end.shape
    strip = rows // 2
    rest_count = space // 2
    core, zh, rest = lax.axis_index("core"), lax.axis_index("zh"), lax.axis_index("rest")
    number = lax.axis_index("x") * 2 + core
    place = zh * rest_count + rest
    order = jnp.where(zh == 0, rest, rest_count - 1 - rest)
    mesh_type = pl.DeviceIdType.MESH
    outward = jnp.where(zh == 0, place + space - 1, place + 1) % space
    inward = jnp.where(zh == 0, place + 1, place + space - 1) % space

    def device(slice_number, target):
        return {
            "x": slice_number // 2, "core": slice_number % 2, "zh": target // rest_count, "rest": target % rest_count,
        }

    native = core == zh
    later, earlier = number < tm - 1, number > 0
    barrier = pltpu.get_barrier_semaphore()
    away = {"core": zh, "zh": 1 - zh, "rest": rest_count - 1 - rest}
    beside = {"core": 1 - core}

    def greet(where):
        pl.semaphore_signal(barrier, inc=1, device_id=where, device_id_type=mesh_type)

    for k in range(2):
        greet({"core": k, "zh": 1 - zh, "rest": rest_count - 1 - rest})
    greet(beside)

    @pl.when(later)
    def _():
        for target in (outward, place, inward):
            greet(device(number + 1, target))

    @pl.when(earlier)
    def _():
        for target in (outward, place, inward):
            greet(device(number - 1, target))

    pl.semaphore_wait(barrier, 3 + jnp.where(later, 3, 0) + jnp.where(earlier, 3, 0))

    def carry_jump(source, n, where):
        return pltpu.make_async_remote_copy(
            src_ref=source, dst_ref=landed.at[core], send_sem=jump_sends.at[n], recv_sem=jump_recvs.at[core],
            device_id=where, device_id_type=mesh_type,
        )

    def await_jump(part):
        pltpu.make_async_remote_copy(
            src_ref=fine.at[0], dst_ref=landed.at[part], send_sem=jump_sends.at[0], recv_sem=jump_recvs.at[part],
            device_id=away, device_id_type=mesh_type,
        ).wait_recv()

    far = carry_jump(fine.at[1], 1, away)
    near = carry_jump(fine.at[0], 0, beside)
    far.start()

    @pl.when(core != zh)
    def _():
        near.start()

    @pl.when(native)
    def _():
        landed[core] = fine[0]
        await_jump(1 - core)

    @pl.when(core != zh)
    def _():
        await_jump(0)
        await_jump(1)

    def outgoing():
        target = number + 1

        def one(n, source, landing, sem, where):
            return pltpu.make_async_remote_copy(
                src_ref=source, dst_ref=landing, send_sem=send_sems.at[n], recv_sem=recv_sems.at[sem],
                device_id=device(target, where), device_id_type=mesh_type,
            )

        outer = jnp.where(order == 0, 0, 1)
        inner = jnp.where(order == rest_count - 1, 1, 0)
        return [
            one(0, out, current.at[:, 8 : 8 + rows, :], 2, place),
            one(1, edge_out.at[0], edge_in.at[outer], outer, outward),
            one(2, edge_out.at[1], edge_in.at[inner], inner, inward),
        ]

    def arrivals():
        def one(source, landing, sem):
            return pltpu.make_async_remote_copy(
                src_ref=source, dst_ref=landing, send_sem=send_sems.at[0], recv_sem=recv_sems.at[sem],
                device_id=device(number - 1, place), device_id_type=mesh_type,
            )

        return [
            one(out, current.at[:, 8 : 8 + rows, :], 2),
            one(edge_out.at[0], edge_in.at[0], 0),
            one(edge_out.at[1], edge_in.at[1], 1),
        ]

    @pl.when(number == 0)
    def _():
        for c in range(3):
            for k in range(2):
                out[c, k * strip : (k + 1) * strip, :] = landed[k, c]

    @pl.when(earlier)
    def _():
        for copy in arrivals():
            copy.wait_recv()
        for c in range(3):
            current[c, 7:8, :] = edge_in[0, c : c + 1, :]
            current[c, 8 + rows : 9 + rows, :] = edge_in[1, c : c + 1, :]
        for at in range(0, rows, 8):
            inside = [current[c, 8 + at : 16 + at, :] for c in range(3)]
            weights = [links[n, at : at + 8, :] for n in range(4)]
            effective = []
            for c in range(3):
                m = inside[c]
                total = weights[0] * (current[c, 7 + at : 15 + at, :] - m)
                total = total + weights[1] * (current[c, 9 + at : 17 + at, :] - m)
                total = total + weights[2] * (pltpu.roll(m, 1, 1) - m)
                total = total + weights[3] * (pltpu.roll(m, grid - 1, 1) - m)
                total = total + field[c, at : at + 8, :]
                effective.append(total - m if c == 2 else total)
            first = cross_of(inside, effective)
            second = cross_of(inside, first)
            k, inner = at // strip, at % strip
            for c in range(3):
                value = -(first[c] + damping * second[c]) * (1.0 / (1.0 + damping * damping))
                moved = inside[c] + FINE * step_time * value
                jump = landed[k, c, inner : inner + 8, :] - coarse_end[c, at : at + 8, :]
                out[c, at : at + 8, :] = moved + jump

    @pl.when(later)
    def _():
        for c in range(3):
            edge_out[0, c : c + 1, :] = out[c, 0:1, :]
            edge_out[1, c : c + 1, :] = out[c, rows - 1 : rows, :]
        copies = outgoing()
        for copy in copies:
            copy.start()
        for copy in copies:
            copy.wait_send()

    far.wait_send()

    @pl.when(core != zh)
    def _():
        near.wait_send()


def sweep(space, tm, fine, coarse_end, field, links):
    _, rows, grid = coarse_end.shape
    f32 = jnp.float32

    def kernel(*refs):
        sweep_kernel(space, tm, *refs)

    return pl.pallas_call(
        kernel,
        out_shape=jax.ShapeDtypeStruct(coarse_end.shape, f32),
        in_specs=[pl.BlockSpec(memory_space=pltpu.VMEM)] * 4,
        out_specs=pl.BlockSpec(memory_space=pltpu.VMEM),
        scratch_shapes=[
            pltpu.VMEM((3, rows + 16, grid), f32),
            pltpu.VMEM((2, 3, rows // 2, grid), f32),
            pltpu.VMEM((2, 8, grid), f32),
            pltpu.VMEM((2, 8, grid), f32),
            pltpu.SemaphoreType.DMA((2,)),
            pltpu.SemaphoreType.DMA((2,)),
            pltpu.SemaphoreType.DMA((3,)),
            pltpu.SemaphoreType.DMA((3,)),
        ],
        compiler_params=pltpu.CompilerParams(
            collective_id=1, has_side_effects=True, vmem_limit_bytes=32 * 1024 * 1024
        ),
    )(fine, coarse_end, field, links)


def links_of(pad_coupling, depth):
    rows = pad_coupling.shape[0] - 2 * depth
    own = pad_coupling[depth : rows + depth]
    flat = jnp.pad(own, ((0, 0), (1, 1)))
    around = [
        pad_coupling[depth - 1 : rows + depth - 1],
        pad_coupling[depth + 1 : rows + depth + 1],
        flat[:, :-2],
        flat[:, 2:],
    ]
    return stiffness * own[None] * jnp.stack(around)


def make_shards(tm, space):
    rest_count = space // 2

    def shards(initial_state, applied_field, coupling):
        rows, _, grid = initial_state.shape
        strip = rows // 2
        depth = tm
        x, core, zh = lax.axis_index("x"), lax.axis_index("core"), lax.axis_index("zh")
        table, fold = sector_tables(grid)

        def inward_order(block):
            return jnp.where(zh == 1, block[::-1], block)

        start = jnp.transpose(inward_order(initial_state), (1, 0, 2))
        field = jnp.transpose(inward_order(applied_field), (1, 0, 2))
        pack = jnp.concatenate([start, field, inward_order(coupling)[None]], axis=0)

        def shift(block, pairs):
            return lax.ppermute(block, ("zh", "rest"), pairs)

        ring = range(1, rest_count)
        before = shift(
            pack[:, rows - depth :], [(i - 1, i) for i in ring] + [(space - i, space - 1 - i) for i in ring]
        )
        after = shift(pack[:, :depth], [(i, i - 1) for i in ring] + [(space - 1 - i, space - i) for i in ring])
        facing = shift(pack[:, rows - depth :], [(rest_count - 1, rest_count), (rest_count, rest_count - 1)])
        place = zh * rest_count + lax.axis_index("rest")
        center = (place == rest_count - 1) | (place == rest_count)
        after = jnp.where(center, facing[:, ::-1], after)
        wide = jnp.concatenate([before, pack, after], axis=1)
        wide_coupling = wide[6]
        wide_field = wide[3:6]
        state = wide[:3]
        mine = theirs = coarse_end = state
        for n in range(tm):
            stepped = jnp.pad(coarse(state, wide_coupling, wide_field[:, 1:-1]), ((0, 0), (1, 1), (0, 0)))
            mine = jnp.where(2 * x + zh == n, state, mine)
            theirs = jnp.where(2 * x + 1 - zh == n, state, theirs)
            coarse_end = jnp.where(2 * x + core == n, stepped, coarse_end)
            state = stepped

        def half_of(block, margin):
            low = block[..., depth - margin : depth + strip + margin, :]
            high = block[..., depth + strip - margin : depth + rows + margin, :]
            return jnp.where(core == 0, low, high)

        tables = [*halves(table), *halves(np.ascontiguousarray(np.transpose(table, (0, 2, 1))))]
        tables += [fold.astype(jnp.bfloat16), np.ascontiguousarray(fold.T).astype(jnp.bfloat16)]
        fine = fine_states(
            space, half_of(mine, 0), half_of(theirs, 0), half_of(wide_field, 0),
            jnp.pad(half_of(wide_coupling, 1), ((7, 7), (0, 0))), tables,
        )
        end = sweep(space, tm, fine, coarse_end[:, depth:-depth], field, links_of(wide_coupling, depth))
        return inward_order(jnp.transpose(end, (1, 0, 2)))[None]

    return shards


def solution(mesh):
    tm, space = mesh.shape["tm"], mesh.shape["space"]
    finer = Mesh(mesh.devices.reshape(tm // 2, 2, 2, space // 2), EVERY)
    rows = ("zh", "rest")
    return jax.shard_map(
        make_shards(tm, space),
        mesh=finer,
        in_specs=(P(rows, None, None), P(rows, None, None), P(rows, None)),
        out_specs=P(("x", "core"), rows, None, None),
        check_vma=False,
    )
```

```python
import functools
import math

import jax
import jax.numpy as jnp
import numpy as np
from jax import lax
from jax.experimental import pallas as pl
from jax.experimental.pallas import tpu as pltpu
from jax.sharding import Mesh, PartitionSpec as P

FINE = 2
step_time = 0.06
damping = 0.02
stiffness = 0.25
thickness = 8.0
PASSES = 1

EVERY = ("x", "core", "zh", "rest")


def sector_tables(grid):
    half = grid // 2
    place = 2 * np.arange(half) - (grid - 1)
    wave = np.arange(grid)
    odd_wave = np.where(wave == 0, grid, wave)
    turn = 4 * grid

    def angle(k):
        return 2.0 * np.pi / turn * ((place[:, None] * k[None, :]) % turn)

    table = np.stack([np.cos(angle(wave)), np.sin(angle(odd_wave))]).astype(np.float32)
    fold = np.zeros((grid, grid), np.float32)
    for i in range(half):
        fold[i, i] = fold[grid - 1 - i, i] = fold[i, half + i] = 1.0
        fold[grid - 1 - i, half + i] = -1.0
    return table, fold


def halves(table):
    high = table.astype(jnp.bfloat16)
    return [high, (table - high.astype(np.float32)).astype(jnp.bfloat16)]


def split(value):
    high = value.astype(jnp.bfloat16)
    return high, (value - high.astype(jnp.float32)).astype(jnp.bfloat16)


def cross_of(a, b):
    return [a[1] * b[2] - a[2] * b[1], a[2] * b[0] - a[0] * b[2], a[0] * b[1] - a[1] * b[0]]


def product(passes, left, right):
    def one(a, b):
        return jnp.dot(a, b, preferred_element_type=jnp.float32)

    value = one(left[0], right[0])
    if passes > 1:
        value = value + one(left[1], right[0])
    if passes > 2:
        value = value + one(left[0], right[1])
    return value


def put(passes, pair, where, value):
    high, low = split(value)
    pair[0][where] = high
    if passes > 1:
        pair[1][where] = low


HALO = 8


def parareal_kernel(
    space, tm,
    pack, table_high, table_low, turned_high, turned_low, fold, unfold,
    out,
    state, wide_field, wide_coupling, wide_links, halo_in, theirs, coarse_end,
    current, rate, base, probe, demag, far_start, far_field, far_coupling, links, far_links, tensors,
    edge_out, edge_in, wide_high, wide_low, send_xy, send_z, land, back, got_xy, got_z,
    plane_high, plane_low, mixed_high, mixed_low,
    jumps_in, arrived, last_out, last_in,
    halo_sems, swap_sems, edge_sems, send_sems, land_sems, back_sems, got_sems,
    jump_sends, jump_recvs, chain_sends, chain_recvs,
):
    _, rows, grid = pack.shape
    strip = rows // 2
    rest_count = space // 2
    half = grid // 2
    multi = rest_count // 4
    width = grid // multi
    core, zh, rest = lax.axis_index("core"), lax.axis_index("zh"), lax.axis_index("rest")
    axis_x = lax.axis_index("x")
    slice_number = axis_x * 2 + core
    place = zh * rest_count + rest
    order = jnp.where(zh == 0, rest, rest_count - 1 - rest)
    number = 2 * order + core
    unit = rest // multi
    share = rest % multi
    row_odd, column_odd = unit // 2, unit % 2
    outward_place = jnp.where(zh == 0, place + space - 1, place + 1) % space
    inward_place = jnp.where(zh == 0, place + 1, place + space - 1) % space
    first_block, last_block = order == 0, order == rest_count - 1
    mirror = rest_count - 1 - rest

    def at_place(core_index, rest_index):
        return {"core": core_index, "rest": rest_index}

    def owner(index):
        spot = index // 2
        return at_place(index % 2, jnp.where(zh == 0, spot, rest_count - 1 - spot))

    def block_at(where):
        return {"zh": where // rest_count, "rest": where % rest_count}

    def in_slice(which, where):
        return {
            "x": which // 2, "core": which % 2, "zh": where // rest_count, "rest": where % rest_count,
        }

    def remote(source, target, send_sem, recv_sem, where):
        return pltpu.make_async_remote_copy(
            src_ref=source, dst_ref=target, send_sem=send_sem, recv_sem=recv_sem,
            device_id=where, device_id_type=pl.DeviceIdType.MESH,
        )

    barrier = pltpu.get_barrier_semaphore()
    later, earlier = slice_number < tm - 1, slice_number > 0

    def greet(where):
        pl.semaphore_signal(barrier, inc=1, device_id=where, device_id_type=pl.DeviceIdType.MESH)

    def greet_group(k, carry):
        greet(owner((number + k) % space))
        return carry

    lax.fori_loop(1, space, greet_group, 0)
    for k in range(2):
        greet({"core": k, "zh": 1 - zh, "rest": mirror})

    @pl.when(later)
    def _():
        for where in (outward_place, place, inward_place):
            greet(in_slice(slice_number + 1, where))

    @pl.when(earlier)
    def _():
        for where in (outward_place, place, inward_place):
            greet(in_slice(slice_number - 1, where))

    pl.semaphore_wait(barrier, space + 1 + jnp.where(later, 3, 0) + jnp.where(earlier, 3, 0))

    to_outward = remote(
        pack.at[:, pl.ds(0, HALO), :], halo_in.at[1], halo_sems.at[0, 0], halo_sems.at[1, 1], block_at(outward_place)
    )
    inner_slot = jnp.where(last_block, 1, 0)
    to_inward = remote(
        pack.at[:, pl.ds(rows - HALO, HALO), :], halo_in.at[inner_slot],
        halo_sems.at[0, 1], halo_sems.at[1, inner_slot], block_at(inward_place),
    )

    def halo_arrival(slot):
        return remote(
            pack.at[:, pl.ds(0, HALO), :], halo_in.at[slot], halo_sems.at[0, 0], halo_sems.at[1, slot],
            block_at(inward_place),
        )

    @pl.when(jnp.logical_not(first_block))
    def _():
        to_outward.start()

    to_inward.start()

    partner = {"zh": 1 - zh, "rest": mirror}
    core_rows = pl.ds(pl.multiple_of(core * strip, strip), strip)
    top = 2 * HALO

    state[0, :, top : top + rows, :] = pack[0:3]
    wide_field[:, top : top + rows, :] = pack[3:6]
    wide_coupling[top : top + rows, :] = pack[6]

    def fill(i, carry):
        at = pl.multiple_of(i * 64, 64)
        slot_rows = at + lax.broadcasted_iota(jnp.int32, (64, width), 0)
        slot_columns = share * width + lax.broadcasted_iota(jnp.int32, (64, width), 1)
        unit_length = 2.0 * math.pi / (2 * grid)

        def parts(odd_rows, odd_columns):
            rows = jnp.where((slot_rows == 0) & (odd_rows == 1), grid, slot_rows)
            columns = jnp.where((slot_columns == 0) & (odd_columns == 1), grid, slot_columns)
            wave_rows = unit_length * rows.astype(jnp.float32)
            wave_columns = unit_length * columns.astype(jnp.float32)
            squared = wave_rows * wave_rows + wave_columns * wave_columns
            nonzero = squared > 0.0
            safe = jnp.where(nonzero, squared, 1.0)
            scaled = jnp.sqrt(safe) * thickness
            film = jnp.where(nonzero, (1.0 - jnp.exp(-scaled)) / scaled, 1.0)
            weight = jnp.where(slot_rows == 0, 1.0, 2.0) * jnp.where(slot_columns == 0, 1.0, 2.0)
            weight = weight * (-1.0 / (4 * grid * grid))
            return wave_rows, wave_columns, film, (1.0 - film) / safe, weight

        @pl.when(core == 1)
        def _():
            wave_rows, wave_columns, _, in_plane, weight = parts(row_odd, column_odd)
            tensors[0, pl.ds(at, 64), :] = in_plane * wave_columns * wave_columns * weight
            mixed = in_plane * wave_columns * wave_rows * weight
            sign = jnp.where((row_odd == column_odd) == (zh == 0), -1.0, 1.0)
            tensors[2, pl.ds(at, 64), :] = jnp.where((slot_rows == 0) | (slot_columns == 0), 0.0, mixed * sign)
            wave_rows, wave_columns, _, in_plane, weight = parts(1 - row_odd, 1 - column_odd)
            tensors[1, pl.ds(at, 64), :] = in_plane * wave_rows * wave_rows * weight

        @pl.when(core == 0)
        def _():
            _, _, film, _, weight = parts(row_odd, column_odd)
            tensors[0, pl.ds(at, 64), :] = film * weight

        return carry

    lax.fori_loop(0, grid // 64, fill, 0)


    def set_halo(at, slot, lines):
        for r, line in enumerate(lines):
            state[0, :, at + r : at + r + 1, :] = halo_in[slot, 0:3, line : line + 1, :]
            wide_field[:, at + r : at + r + 1, :] = halo_in[slot, 3:6, line : line + 1, :]
            wide_coupling[at + r : at + r + 1, :] = halo_in[slot, 6, line : line + 1, :]

    def set_block(at, slot):
        state[0, :, at : at + HALO, :] = halo_in[slot, 0:3]
        wide_field[:, at : at + HALO, :] = halo_in[slot, 3:6]
        wide_coupling[at : at + HALO, :] = halo_in[slot, 6]

    @pl.when(first_block)
    def _():
        state[0, :, HALO : top, :] = jnp.zeros((3, HALO, grid), jnp.float32)
        wide_field[:, HALO : top, :] = jnp.zeros((3, HALO, grid), jnp.float32)
        wide_coupling[HALO : top, :] = jnp.zeros((HALO, grid), jnp.float32)

    @pl.when(jnp.logical_not(first_block))
    def _():
        halo_arrival(0).wait_recv()
        set_block(HALO, 0)

    halo_arrival(1).wait_recv()

    @pl.when(last_block)
    def _():
        set_halo(top + rows, 1, list(range(HALO))[::-1])

    @pl.when(jnp.logical_not(last_block))
    def _():
        set_block(top + rows, 1)

    for at in (HALO - 1, top + rows + HALO):
        edge = jnp.zeros((1, grid), jnp.float32)
        wide_coupling[at : at + 1, :] = edge
        for n in range(2):
            for c in range(3):
                state[n, c, at : at + 1, :] = edge

    def make_links(target, first, last, source):
        lane = lax.broadcasted_iota(jnp.int32, (8, grid), 1)
        for at in range(first, last, 8):
            centre = source[at : at + 8, :]
            own = stiffness * centre
            target[0, at : at + 8, :] = own * source[at - 1 : at + 7, :]
            target[1, at : at + 8, :] = own * source[at + 1 : at + 9, :]
            target[2, at : at + 8, :] = jnp.where(lane == 0, 0.0, own * pltpu.roll(centre, 1, 1))
            target[3, at : at + 8, :] = jnp.where(lane == grid - 1, 0.0, own * pltpu.roll(centre, grid - 1, 1))

    make_links(wide_links, HALO, top + rows + HALO, wide_coupling)

    def exchange(read, weights, at):
        total = []
        inside = []
        for c in range(3):
            m = read(c, at)
            value = weights[0] * (read(c, at - 1) - m)
            value = value + weights[1] * (read(c, at + 1) - m)
            value = value + weights[2] * (pltpu.roll(m, 1, 1) - m)
            total.append(value + weights[3] * (pltpu.roll(m, grid - 1, 1) - m))
            inside.append(m)
        return inside, total

    def torque_of(inside, effective):
        turned = cross_of(inside, effective)
        again = cross_of(inside, turned)
        return [-(turned[c] + damping * again[c]) * (1.0 / (1.0 + damping * damping)) for c in range(3)]

    def coarse_step(n):
        before, after = n % 2, (n + 1) % 2

        for at in range(HALO, top + rows + HALO, 8):
            weights = [wide_links[k, at : at + 8, :] for k in range(4)]
            inside, total = exchange(lambda c, where: state[before, c, where : where + 8, :], weights, at)
            effective = [total[c] + wide_field[c, at : at + 8, :] for c in range(3)]
            effective[2] = effective[2] - inside[2]
            moved = torque_of(inside, effective)
            for c in range(3):
                state[after, c, at : at + 8, :] = inside[c] + FINE * step_time * moved[c]

    def native(n):
        return state[n % 2, :, pl.ds(pl.multiple_of(top + core * strip, 8), strip), :]

    def step_body(n, carry):
        coarse_step(n)
        return carry

    lax.fori_loop(0, 2 * axis_x, step_body, 0)
    field_source = pack.at[3:6, core_rows, :]
    coupling_source = wide_coupling.at[pl.ds(pl.multiple_of(HALO + core * strip, 8), strip + 2 * HALO), :]
    swaps = [
        remote(source, target, swap_sems.at[0, n], swap_sems.at[1, n], partner)
        for n, (source, target) in enumerate(
            ((theirs, far_start), (field_source, far_field), (coupling_source, far_coupling))
        )
    ]

    @pl.when(zh == 1)
    def _():
        theirs[...] = native(0)
        swaps[0].start()

    @pl.when(zh == 0)
    def _():
        base[0] = native(0)

    coarse_step(0)

    @pl.when(zh == 0)
    def _():
        theirs[...] = native(1)
        swaps[0].start()

    @pl.when(zh == 1)
    def _():
        base[0] = native(1)

    swaps[1].start()
    swaps[2].start()

    @pl.when(core == 0)
    def _():
        coarse_end[...] = state[1, :, top : top + rows, :]

    @pl.when(core == 1)
    def _():
        coarse_step(1)
        coarse_end[...] = state[0, :, top : top + rows, :]


    for k in range(4):
        links[0, k] = wide_links[k, pl.ds(pl.multiple_of(top + core * strip, 8), strip), :]
    swaps[0].wait()
    base[1] = far_start[...]
    current[:, :, 8 : 8 + strip, :] = base[...]
    probe[...] = base[...]

    def to_unit(kind, r):
        target = (rest + r) % rest_count
        if kind == 1:
            source, landing = send_xy.at[target // multi], land.at[:, pl.ds(number * strip, strip), :]
        else:
            source, landing = send_z.at[target // multi], land.at[0, pl.ds(number * strip, strip), :]
        return remote(source, landing, send_sems.at[kind, r], land_sems.at[number], at_place(kind, target))

    def landed(kind, index):
        if kind == 1:
            source, landing = send_xy.at[0], land.at[:, pl.ds(index * strip, strip), :]
        else:
            source, landing = send_z.at[0], land.at[0, pl.ds(index * strip, strip), :]
        return remote(source, landing, send_sems.at[kind, 0], land_sems.at[index], owner(index))

    def to_owner(kind, k):
        index = (number + k) % space
        if kind == 1:
            source, landing = back.at[:, pl.ds(index * strip, strip), :], got_xy.at[rest]
        else:
            source, landing = back.at[0, pl.ds(index * strip, strip), :], got_z.at[rest]
        return remote(source, landing, back_sems.at[k], got_sems.at[kind, rest], owner(index))

    def gotten(kind, r):
        if kind == 1:
            source, landing = back.at[:, pl.ds(0, strip), :], got_xy.at[r]
        else:
            source, landing = back.at[0, pl.ds(0, strip), :], got_z.at[r]
        return remote(source, landing, back_sems.at[0], got_sems.at[kind, r], at_place(kind, r))

    def transform(kind, passes):
        planes = [(row_odd, column_odd), (1 - row_odd, 1 - column_odd)] if kind == 1 else [(row_odd, column_odd)]
        columns = pl.ds(pl.multiple_of(share * width, width), width)
        for n, (_, odd) in enumerate(planes):
            spectrum = product(
                passes, split(land[n]), (table_high[odd, :, columns], table_low[odd, :, columns])
            )
            put(passes, (plane_high, plane_low), n, spectrum)
        step = half

        def mix(i, carry):
            at = pl.multiple_of(i * step, step)
            lines = pl.ds(at, step)
            both = [
                product(
                    passes, (turned_high[odd, lines, :], turned_low[odd, lines, :]), (plane_high[n], plane_low[n])
                )
                for n, (odd, _) in enumerate(planes)
            ]
            if kind == 1:
                cross_term = tensors[2, lines, :]
                values = [
                    tensors[0, lines, :] * both[0] + cross_term * both[1],
                    cross_term * both[0] + tensors[1, lines, :] * both[1],
                ]
            else:
                values = [tensors[0, lines, :] * both[0]]
            for n, value in enumerate(values):
                put(passes, (mixed_high, mixed_low), (n, lines), value)
            return carry

        lax.fori_loop(0, grid // step, mix, 0)
        for n, (odd_rows, odd_columns) in enumerate(planes):
            film = product(
                passes, (table_high[odd_rows], table_low[odd_rows]), (mixed_high[n], mixed_low[n])
            )
            back[n] = product(
                passes, split(film), (turned_high[odd_columns, columns, :], turned_low[odd_columns, columns, :])
            )

    def unit_work(kind, passes):
        @pl.when(core == kind)
        def _():
            def take(k, carry):
                landed(kind, (number + k) % space).wait_recv()
                return carry

            lax.fori_loop(1, space, take, 0)
            transform(kind, passes)

            def push(k, carry):
                to_owner(kind, k).start()
                return carry

            lax.fori_loop(1, space, push, 0)
            own = pl.ds(pl.multiple_of(number * strip, strip), strip)
            if kind == 1:
                got_xy[rest] = back[:, own, :]
            else:
                got_z[rest] = back[0, own, :]

    def unit_end(kind):
        @pl.when(core == kind)
        def _():
            def drain(k, carry):
                to_owner(kind, k).wait_send()
                return carry

            lax.fori_loop(1, space, drain, 0)

    def evaluate(parity, passes, first):
        for t in range(2):
            for c in range(3):
                edge_out[0, 3 * t + c : 3 * t + c + 1, :] = current[t, c, 8:9, :]
                edge_out[1, 3 * t + c : 3 * t + c + 1, :] = current[t, c, 7 + strip : 8 + strip, :]
        outward = remote(
            edge_out.at[0], edge_in.at[parity, 1], edge_sems.at[parity, 0], edge_sems.at[parity, 1], owner((number + space - 1) % space)
        )
        inward = remote(
            edge_out.at[1], edge_in.at[parity, 0], edge_sems.at[parity, 2], edge_sems.at[parity, 3], owner((number + 1) % space)
        )
        fold_passes = min(passes, 2)
        for c in range(3):
            near, far = probe[0, c], probe[1, c]
            for p, value in enumerate((near + far, near - far)):
                put(fold_passes, (wide_high, wide_low), pl.ds((3 * p + c) * strip, strip), value)
        folded = product(fold_passes, (wide_high[...], wide_low[...]), (fold[...],))
        for p in range(2):
            for q in range(2):
                for c in range(3):
                    piece = folded[(3 * p + c) * strip : (3 * p + c + 1) * strip, q * half : (q + 1) * half]
                    if c == 0:
                        send_xy[2 * p + q, 0] = piece
                    elif c == 1:
                        send_xy[2 * (1 - p) + 1 - q, 1] = piece
                    else:
                        send_z[2 * p + q] = piece

        def launch(r, carry):
            for kind in range(2):
                @pl.when((core != kind) | (r != 0))
                def _(kind=kind):
                    to_unit(kind, r).start()

            return carry

        lax.fori_loop(0, rest_count, launch, 0)
        outward.start()
        inward.start()
        own = pl.ds(pl.multiple_of(number * strip, strip), strip)

        @pl.when(core == 1)
        def _():
            land[:, own, :] = send_xy[unit]

        @pl.when(core == 0)
        def _():
            land[0, own, :] = send_z[unit]

        unit_work(1, passes)
        unit_work(0, passes)

        def settle(r, carry):
            for kind in range(2):
                @pl.when((core != kind) | (r != 0))
                def _(kind=kind):
                    to_unit(kind, r).wait_send()
                    gotten(kind, (rest + r) % rest_count).wait_recv()

            return carry

        lax.fori_loop(0, rest_count, settle, 0)
        outward.wait()
        inward.wait()
        for p in range(2):
            for q in range(2):
                for c in range(3):
                    source = 2 * (1 - p) + 1 - q if c == 1 else 2 * p + q
                    value = None
                    for k in range(multi):
                        piece = got_z[source * multi + k] if c == 2 else got_xy[source * multi + k, c]
                        value = piece if value is None else value + piece
                    where = (pl.ds((3 * p + c) * strip, strip), pl.ds(q * half, half))
                    put(fold_passes, (wide_high, wide_low), where, value)
        unfolded = product(fold_passes, (wide_high[...], wide_low[...]), (unfold[...],))
        for c in range(3):
            even = unfolded[c * strip : (c + 1) * strip]
            odd = unfolded[(3 + c) * strip : (4 + c) * strip]
            for t, value in enumerate((even + odd, even - odd)):
                if first:
                    demag[0, t, c] = value
                    demag[1, t, c] = value
                elif parity == 0:
                    moved = demag[0, t, c] + value
                    demag[0, t, c] = moved
                    demag[1, t, c] = moved
                else:
                    demag[1, t, c] = demag[0, t, c] + value
        if first:
            for swap in swaps[1:]:
                swap.wait()
            make_links(far_links, HALO, HALO + strip, far_coupling)
            links[1] = far_links[:, HALO : HALO + strip, :]
        unit_end(1)
        unit_end(0)
        last = number == space - 1
        for t in range(2):
            for c in range(3):
                current[t, c, 7:8, :] = edge_in[parity, 0, 3 * t + c : 3 * t + c + 1, :]
                facing = current[1 - t, c, 7 + strip : 8 + strip, :]
                arrived = edge_in[parity, 1, 3 * t + c : 3 * t + c + 1, :]
                current[t, c, 8 + strip : 9 + strip, :] = jnp.where(last, facing, arrived)
        for t in range(2):
            applied = (wide_field.at[:, pl.ds(pl.multiple_of(top + core * strip, 8), strip), :], far_field)[t]
            for at in range(0, strip, 8):
                rows_here = slice(at, at + 8)
                weights = [links[t, n, rows_here, :] for n in range(4)]
                inside, total = exchange(lambda c, where: current[t, c, where : where + 8, :], weights, 8 + at)
                effective = [total[c] + demag[1, t, c, rows_here, :] + applied[c, rows_here, :] for c in range(3)]
                moved = torque_of(inside, effective)
                for c in range(3):
                    if parity == 0:
                        rate[t, c, rows_here, :] = moved[c]
                        probe[t, c, rows_here, :] = step_time * moved[c]
                    else:
                        change = 0.5 * step_time * (rate[t, c, rows_here, :] + moved[c])
                        probe[t, c, rows_here, :] = change
                        base[t, c, rows_here, :] = base[t, c, rows_here, :] + change
        if parity == 0:
            current[:, :, 8 : 8 + strip, :] = base[...] + probe[...]
        else:
            current[:, :, 8 : 8 + strip, :] = base[...]

    evaluate(0, 3, True)

    def fine_step(i, carry):
        evaluate(1, PASSES, False)
        evaluate(0, PASSES, False)
        return carry

    lax.fori_loop(1, FINE, fine_step, 0)
    evaluate(1, PASSES, False)

    direct = core == zh
    away = {"core": zh, "zh": 1 - zh, "rest": mirror}
    beside = {"core": 1 - core}

    def carry_jump(t, where):
        return remote(base.at[t], jumps_in.at[core], jump_sends.at[t], jump_recvs.at[core], where)

    def await_jump(part):
        remote(base.at[0], jumps_in.at[part], jump_sends.at[0], jump_recvs.at[part], away).wait_recv()

    far, near = carry_jump(1, away), carry_jump(0, beside)
    far.start()

    @pl.when(jnp.logical_not(direct))
    def _():
        near.start()
        await_jump(0)
        await_jump(1)

    @pl.when(direct)
    def _():
        jumps_in[core] = base[0]
        await_jump(1 - core)

    outer = jnp.where(first_block, 0, 1)
    inner = jnp.where(last_block, 1, 0)
    outgoing = [
        remote(source, target, chain_sends.at[n], chain_recvs.at[sem], in_slice(slice_number + 1, where))
        for n, (source, target, sem, where) in enumerate((
            (out, arrived.at[:, pl.ds(8, rows), :], 2, place),
            (last_out.at[0], last_in.at[outer], outer, outward_place),
            (last_out.at[1], last_in.at[inner], inner, inward_place),
        ))
    ]
    arrivals = [
        remote(source, target, chain_sends.at[0], chain_recvs.at[sem], in_slice(slice_number - 1, place))
        for source, target, sem in (
            (out, arrived.at[:, pl.ds(8, rows), :], 2),
            (last_out.at[0], last_in.at[0], 0),
            (last_out.at[1], last_in.at[1], 1),
        )
    ]

    @pl.when(slice_number == 0)
    def _():
        for c in range(3):
            for k in range(2):
                out[c, k * strip : (k + 1) * strip, :] = jumps_in[k, c]

    @pl.when(earlier)
    def _():
        for copy in arrivals:
            copy.wait_recv()
        for c in range(3):
            arrived[c, 7:8, :] = last_in[0, c : c + 1, :]
            arrived[c, 8 + rows : 9 + rows, :] = last_in[1, c : c + 1, :]
        for at in range(0, rows, 8):
            weights = [wide_links[n, top + at : top + at + 8, :] for n in range(4)]
            inside, total = exchange(lambda c, where: arrived[c, where : where + 8, :], weights, 8 + at)
            effective = [total[c] + wide_field[c, top + at : top + at + 8, :] for c in range(3)]
            effective[2] = effective[2] - inside[2]
            moved = torque_of(inside, effective)
            k, within = at // strip, at % strip
            for c in range(3):
                jump = jumps_in[k, c, within : within + 8, :] - coarse_end[c, at : at + 8, :]
                out[c, at : at + 8, :] = inside[c] + FINE * step_time * moved[c] + jump

    @pl.when(later)
    def _():
        for c in range(3):
            last_out[0, c : c + 1, :] = out[c, 0:1, :]
            last_out[1, c : c + 1, :] = out[c, rows - 1 : rows, :]
        for copy in outgoing:
            copy.start()
        for copy in outgoing:
            copy.wait_send()

    far.wait_send()

    @pl.when(jnp.logical_not(direct))
    def _():
        near.wait_send()

    @pl.when(jnp.logical_not(first_block))
    def _():
        to_outward.wait_send()

    to_inward.wait_send()


def parareal(space, tm, pack, tables):
    _, rows, grid = pack.shape
    strip = rows // 2
    half = grid // 2
    rest_count = space // 2
    width = grid * 4 // rest_count
    f32, bf16 = jnp.float32, jnp.bfloat16
    operands = [pack, *tables]
    return pl.pallas_call(
        functools.partial(parareal_kernel, space, tm),
        out_shape=jax.ShapeDtypeStruct((3, rows, grid), f32),
        in_specs=[pl.BlockSpec(memory_space=pltpu.VMEM)] * len(operands),
        out_specs=pl.BlockSpec(memory_space=pltpu.VMEM),
        scratch_shapes=[
            pltpu.VMEM((2, 3, rows + 4 * HALO, grid), f32),
            pltpu.VMEM((3, rows + 4 * HALO, grid), f32),
            pltpu.VMEM((rows + 4 * HALO, grid), f32),
            pltpu.VMEM((4, rows + 4 * HALO, grid), f32),
            pltpu.VMEM((2, 7, HALO, grid), f32),
            pltpu.VMEM((3, strip, grid), f32),
            pltpu.VMEM((3, rows, grid), f32),
            pltpu.VMEM((2, 3, strip + 16, grid), f32),
            pltpu.VMEM((2, 3, strip, grid), f32),
            pltpu.VMEM((2, 3, strip, grid), f32),
            pltpu.VMEM((2, 3, strip, grid), f32),
            pltpu.VMEM((2, 2, 3, strip, grid), f32),
            pltpu.VMEM((3, strip, grid), f32),
            pltpu.VMEM((3, strip, grid), f32),
            pltpu.VMEM((strip + 16, grid), f32),
            pltpu.VMEM((2, 4, strip, grid), f32),
            pltpu.VMEM((4, strip + 16, grid), f32),
            pltpu.VMEM((3, grid, width), f32),
            pltpu.VMEM((2, 8, grid), f32),
            pltpu.VMEM((2, 2, 8, grid), f32),
            pltpu.VMEM((6 * strip, grid), bf16),
            pltpu.VMEM((6 * strip, grid), bf16),
            pltpu.VMEM((4, 2, strip, half), f32),
            pltpu.VMEM((4, strip, half), f32),
            pltpu.VMEM((2, half, half), f32),
            pltpu.VMEM((2, half, half), f32),
            pltpu.VMEM((rest_count, 2, strip, half), f32),
            pltpu.VMEM((rest_count, strip, half), f32),
            pltpu.VMEM((2, half, width), bf16),
            pltpu.VMEM((2, half, width), bf16),
            pltpu.VMEM((2, grid, width), bf16),
            pltpu.VMEM((2, grid, width), bf16),
            pltpu.VMEM((2, 3, strip, grid), f32),
            pltpu.VMEM((3, rows + 16, grid), f32),
            pltpu.VMEM((2, 8, grid), f32),
            pltpu.VMEM((2, 8, grid), f32),
            pltpu.SemaphoreType.DMA((2, 2)),
            pltpu.SemaphoreType.DMA((2, 3)),
            pltpu.SemaphoreType.DMA((2, 4)),
            pltpu.SemaphoreType.DMA((2, rest_count)),
            pltpu.SemaphoreType.DMA((space,)),
            pltpu.SemaphoreType.DMA((space,)),
            pltpu.SemaphoreType.DMA((2, rest_count)),
            pltpu.SemaphoreType.DMA((2,)),
            pltpu.SemaphoreType.DMA((2,)),
            pltpu.SemaphoreType.DMA((3,)),
            pltpu.SemaphoreType.DMA((3,)),
        ],
        compiler_params=pltpu.CompilerParams(
            collective_id=0, has_side_effects=True, vmem_limit_bytes=56 * 1024 * 1024
        ),
    )(*operands)


def make_shards(tm, space):
    def shards(initial_state, applied_field, coupling):
        grid = initial_state.shape[2]
        zh = lax.axis_index("zh")
        table, fold = sector_tables(grid)

        def inward_order(block):
            return jnp.where(zh == 1, block[::-1], block)

        start = jnp.transpose(inward_order(initial_state), (1, 0, 2))
        field = jnp.transpose(inward_order(applied_field), (1, 0, 2))
        pack = jnp.concatenate([start, field, inward_order(coupling)[None]], axis=0)
        tables = [*halves(table), *halves(np.ascontiguousarray(np.transpose(table, (0, 2, 1))))]
        tables += [fold.astype(jnp.bfloat16), np.ascontiguousarray(fold.T).astype(jnp.bfloat16)]
        end = parareal(space, tm, pack, tables)
        return inward_order(jnp.transpose(end, (1, 0, 2)))[None]

    return shards


def solution(mesh):
    tm, space = mesh.shape["tm"], mesh.shape["space"]
    finer = Mesh(mesh.devices.reshape(tm // 2, 2, 2, space // 2), EVERY)
    rows = ("zh", "rest")
    return jax.shard_map(
        make_shards(tm, space),
        mesh=finer,
        in_specs=(P(rows, None, None), P(rows, None, None), P(rows, None)),
        out_specs=P(("x", "core"), rows, None, None),
        check_vma=False,
    )
```

```python
import functools
import math

import jax
import jax.numpy as jnp
import numpy as np
from jax import lax
from jax.experimental import pallas as pl
from jax.experimental.pallas import tpu as pltpu
from jax.sharding import Mesh, PartitionSpec as P

FINE = 2
step_time = 0.06
damping = 0.02
stiffness = 0.25
thickness = 8.0
PASSES = 1

EVERY = ("x", "core", "zh", "rest")


def sector_tables(grid):
    half = grid // 2
    place = 2 * np.arange(half) - (grid - 1)
    wave = np.arange(grid)
    odd_wave = np.where(wave == 0, grid, wave)
    turn = 4 * grid

    def angle(k):
        return 2.0 * np.pi / turn * ((place[:, None] * k[None, :]) % turn)

    table = np.stack([np.cos(angle(wave)), np.sin(angle(odd_wave))]).astype(np.float32)
    fold = np.zeros((grid, grid), np.float32)
    for i in range(half):
        fold[i, i] = fold[grid - 1 - i, i] = fold[i, half + i] = 1.0
        fold[grid - 1 - i, half + i] = -1.0
    return table, fold


def halves(table):
    high = table.astype(jnp.bfloat16)
    return [high, (table - high.astype(np.float32)).astype(jnp.bfloat16)]


def split(value):
    high = value.astype(jnp.bfloat16)
    return high, (value - high.astype(jnp.float32)).astype(jnp.bfloat16)


def cross_of(a, b):
    return [a[1] * b[2] - a[2] * b[1], a[2] * b[0] - a[0] * b[2], a[0] * b[1] - a[1] * b[0]]


def product(passes, left, right):
    def one(a, b):
        return jnp.dot(a, b, preferred_element_type=jnp.float32)

    value = one(left[0], right[0])
    if passes > 1:
        value = value + one(left[1], right[0])
    if passes > 2:
        value = value + one(left[0], right[1])
    return value


def put(passes, pair, where, value):
    high, low = split(value)
    pair[0][where] = high
    if passes > 1:
        pair[1][where] = low


VMEM_LIMIT = 66_600_000
HALO = 8
EARLY = 2
TABLES = 9


def parareal_kernel(
    space, tm,
    *refs,
):
    sources, out, rest_refs = refs[:TABLES], refs[TABLES], refs[TABLES + 1 :]
    copies_in, rest_refs = rest_refs[: TABLES + 1], rest_refs[TABLES + 1 :]
    (
        start_in, field_in, coupling_in, table_high, table_low, turned_high, turned_low, fold, unfold, table_sems,
    ) = copies_in
    (
        state, wide_field, wide_coupling, wide_links, halo_out, halo_in, theirs, coarse_end,
        current, rate, base, probe, demag, far_start, far_field, far_coupling, links, far_links, tensors,
        edge_out, edge_in, wide_high, wide_low, send, land, back, got,
        plane_high, plane_low, mixed_high, mixed_low,
        jumps_in, arrived, last_out, last_in,
        halo_sems, swap_sems, edge_sems, send_sems, land_sems, back_sems, got_sems,
        jump_sends, jump_recvs, chain_sends, chain_recvs,
    ) = rest_refs
    loads = [
        pltpu.make_async_copy(source, target, table_sems.at[n])
        for n, (source, target) in enumerate(zip(sources, copies_in[:TABLES]))
    ]
    for load in loads:
        load.start()
    _, rows, grid = start_in.shape
    strip = rows // 2
    rest_count = space // 2
    half = grid // 2
    multi = rest_count // 4
    width = grid // multi
    core, zh, rest = lax.axis_index("core"), lax.axis_index("zh"), lax.axis_index("rest")
    axis_x = lax.axis_index("x")
    slice_number = axis_x * 2 + core
    place = zh * rest_count + rest
    order = jnp.where(zh == 0, rest, rest_count - 1 - rest)
    number = 2 * order + core
    unit = rest // multi
    share = rest % multi
    row_odd, column_odd = unit // 2, unit % 2
    outward_place = jnp.where(zh == 0, place + space - 1, place + 1) % space
    inward_place = jnp.where(zh == 0, place + 1, place + space - 1) % space
    first_block, last_block = order == 0, order == rest_count - 1
    mirror = rest_count - 1 - rest

    def at_place(core_index, rest_index):
        return {"core": core_index, "rest": rest_index}

    def owner(index):
        spot = index // 2
        return at_place(index % 2, jnp.where(zh == 0, spot, rest_count - 1 - spot))

    def block_at(where):
        return {"zh": where // rest_count, "rest": where % rest_count}

    def in_slice(which, where):
        return {
            "x": which // 2, "core": which % 2, "zh": where // rest_count, "rest": where % rest_count,
        }

    def remote(source, target, send_sem, recv_sem, where):
        return pltpu.make_async_remote_copy(
            src_ref=source, dst_ref=target, send_sem=send_sem, recv_sem=recv_sem,
            device_id=where, device_id_type=pl.DeviceIdType.MESH,
        )

    barrier = pltpu.get_barrier_semaphore()
    later, earlier = slice_number < tm - 1, slice_number > 0

    def greet(where):
        pl.semaphore_signal(barrier, inc=1, device_id=where, device_id_type=pl.DeviceIdType.MESH)

    def greet_group(k, carry):
        greet(owner((number + k) % space))
        return carry

    lax.fori_loop(1, space, greet_group, 0)
    for k in range(2):
        greet({"core": k, "zh": 1 - zh, "rest": mirror})

    @pl.when(later)
    def _():
        for where in (outward_place, place, inward_place):
            greet(in_slice(slice_number + 1, where))

    @pl.when(earlier)
    def _():
        for where in (outward_place, place, inward_place):
            greet(in_slice(slice_number - 1, where))

    core_rows = pl.ds(pl.multiple_of(2 * HALO + core * strip, 8), strip)
    top = 2 * HALO
    tiles = rows // 8
    sublane = lax.broadcasted_iota(jnp.int32, (8, grid), 0)

    def flipped(value):
        for k in (1, 2, 4):
            value = jnp.where(
                sublane // k % 2 == 1, pltpu.roll(value, k, 0), pltpu.roll(value, 8 - k, 0)
            )
        return value

    def natural(c, at):
        if c < 3:
            return start_in[c, at : at + 8, :]
        return field_in[c - 3, at : at + 8, :] if c < 6 else coupling_in[at : at + 8, :]

    def keep(c, at, value):
        lines = slice(top + at, top + at + 8)
        if c < 3:
            state[0, c, lines, :] = value
        elif c < 6:
            wide_field[c - 3, lines, :] = value
        else:
            wide_coupling[lines, :] = value

    for load in loads[:3]:
        load.wait()

    @pl.when(zh == 0)
    def _():
        for c in range(7):
            for t in range(tiles):
                keep(c, 8 * t, natural(c, 8 * t))
            halo_out[0, c] = natural(c, 0)
            halo_out[1, c] = natural(c, rows - 8)

    @pl.when(zh == 1)
    def _():
        for c in range(7):
            for t in range(tiles):
                value = flipped(natural(c, rows - 8 - 8 * t))
                keep(c, 8 * t, value)
                if t == 0:
                    halo_out[0, c] = value
                if t == tiles - 1:
                    halo_out[1, c] = value

    pl.semaphore_wait(barrier, space + 1 + jnp.where(later, 3, 0) + jnp.where(earlier, 3, 0))

    to_outward = remote(
        halo_out.at[0], halo_in.at[1], halo_sems.at[0, 0], halo_sems.at[1, 1], block_at(outward_place)
    )
    inner_slot = jnp.where(last_block, 1, 0)
    to_inward = remote(
        halo_out.at[1], halo_in.at[inner_slot],
        halo_sems.at[0, 1], halo_sems.at[1, inner_slot], block_at(inward_place),
    )

    def halo_arrival(slot):
        return remote(
            halo_out.at[0], halo_in.at[slot], halo_sems.at[0, 0], halo_sems.at[1, slot],
            block_at(inward_place),
        )

    @pl.when(jnp.logical_not(first_block))
    def _():
        to_outward.start()

    to_inward.start()

    partner = {"zh": 1 - zh, "rest": mirror}
    coupling_source = wide_coupling.at[pl.ds(pl.multiple_of(HALO + core * strip, 8), strip + 2 * HALO), :]
    start_swaps = [
        remote(theirs.at[c], far_start.at[c], swap_sems.at[0, c], swap_sems.at[1, c], partner) for c in range(3)
    ]
    field_swaps = [
        remote(
            wide_field.at[c, core_rows, :], far_field.at[c], swap_sems.at[0, 3 + c], swap_sems.at[1, 3 + c], partner
        )
        for c in range(3)
    ]
    coupling_swap = remote(coupling_source, far_coupling, swap_sems.at[0, 6], swap_sems.at[1, 6], partner)
    for copy in field_swaps[:EARLY]:
        copy.start()


    def set_halo(at, slot, lines):
        for r, line in enumerate(lines):
            state[0, :, at + r : at + r + 1, :] = halo_in[slot, 0:3, line : line + 1, :]
            wide_field[:, at + r : at + r + 1, :] = halo_in[slot, 3:6, line : line + 1, :]
            wide_coupling[at + r : at + r + 1, :] = halo_in[slot, 6, line : line + 1, :]

    def set_block(at, slot):
        state[0, :, at : at + HALO, :] = halo_in[slot, 0:3]
        wide_field[:, at : at + HALO, :] = halo_in[slot, 3:6]
        wide_coupling[at : at + HALO, :] = halo_in[slot, 6]

    @pl.when(first_block)
    def _():
        state[0, :, HALO : top, :] = jnp.zeros((3, HALO, grid), jnp.float32)
        wide_field[:, HALO : top, :] = jnp.zeros((3, HALO, grid), jnp.float32)
        wide_coupling[HALO : top, :] = jnp.zeros((HALO, grid), jnp.float32)

    @pl.when(jnp.logical_not(first_block))
    def _():
        halo_arrival(0).wait_recv()
        set_block(HALO, 0)

    halo_arrival(1).wait_recv()

    @pl.when(last_block)
    def _():
        set_halo(top + rows, 1, list(range(HALO))[::-1])

    @pl.when(jnp.logical_not(last_block))
    def _():
        set_block(top + rows, 1)

    for at in (HALO - 1, top + rows + HALO):
        edge = jnp.zeros((1, grid), jnp.float32)
        wide_coupling[at : at + 1, :] = edge
        for n in range(2):
            for c in range(3):
                state[n, c, at : at + 1, :] = edge

    def make_links(target, first, last, source):
        lane = lax.broadcasted_iota(jnp.int32, (8, grid), 1)
        for at in range(first, last, 8):
            centre = source[at : at + 8, :]
            own = stiffness * centre
            target[0, at : at + 8, :] = own * source[at - 1 : at + 7, :]
            target[1, at : at + 8, :] = own * source[at + 1 : at + 9, :]
            target[2, at : at + 8, :] = jnp.where(lane == 0, 0.0, own * pltpu.roll(centre, 1, 1))
            target[3, at : at + 8, :] = jnp.where(lane == grid - 1, 0.0, own * pltpu.roll(centre, grid - 1, 1))

    make_links(wide_links, HALO, top + rows + HALO, wide_coupling)

    def exchange(read, weights, at):
        total = []
        inside = []
        for c in range(3):
            m = read(c, at)
            value = weights[0] * (read(c, at - 1) - m)
            value = value + weights[1] * (read(c, at + 1) - m)
            value = value + weights[2] * (pltpu.roll(m, 1, 1) - m)
            total.append(value + weights[3] * (pltpu.roll(m, grid - 1, 1) - m))
            inside.append(m)
        return inside, total

    def torque_of(inside, effective):
        turned = cross_of(inside, effective)
        again = cross_of(inside, turned)
        return [-(turned[c] + damping * again[c]) * (1.0 / (1.0 + damping * damping)) for c in range(3)]

    def coarse_step(n):
        before, after = n % 2, (n + 1) % 2

        for at in range(HALO, top + rows + HALO, 8):
            weights = [wide_links[k, at : at + 8, :] for k in range(4)]
            inside, total = exchange(lambda c, where: state[before, c, where : where + 8, :], weights, at)
            effective = [total[c] + wide_field[c, at : at + 8, :] for c in range(3)]
            effective[2] = effective[2] - inside[2]
            moved = torque_of(inside, effective)
            for c in range(3):
                state[after, c, at : at + 8, :] = inside[c] + FINE * step_time * moved[c]

    def native(n):
        return state[n % 2, :, pl.ds(pl.multiple_of(top + core * strip, 8), strip), :]

    def step_pair(n, carry):
        coarse_step(0)
        coarse_step(1)
        return carry

    lax.fori_loop(0, axis_x, step_pair, 0)
    def send_start():
        for copy in start_swaps:
            copy.start()

    @pl.when(zh == 1)
    def _():
        theirs[...] = native(0)
        send_start()

    @pl.when(zh == 0)
    def _():
        base[0] = native(0)

    coarse_step(0)

    @pl.when(zh == 0)
    def _():
        theirs[...] = native(1)
        send_start()

    @pl.when(zh == 1)
    def _():
        base[0] = native(1)

    def fill(i, carry):
        at = pl.multiple_of(i * 64, 64)
        slot_rows = at + lax.broadcasted_iota(jnp.int32, (64, width), 0)
        slot_columns = share * width + lax.broadcasted_iota(jnp.int32, (64, width), 1)
        unit_length = 2.0 * math.pi / (2 * grid)

        def parts(odd_rows, odd_columns):
            rows = jnp.where((slot_rows == 0) & (odd_rows == 1), grid, slot_rows)
            columns = jnp.where((slot_columns == 0) & (odd_columns == 1), grid, slot_columns)
            wave_rows = unit_length * rows.astype(jnp.float32)
            wave_columns = unit_length * columns.astype(jnp.float32)
            squared = wave_rows * wave_rows + wave_columns * wave_columns
            nonzero = squared > 0.0
            safe = jnp.where(nonzero, squared, 1.0)
            scaled = jnp.sqrt(safe) * thickness
            film = jnp.where(nonzero, (1.0 - jnp.exp(-scaled)) / scaled, 1.0)
            weight = jnp.where(slot_rows == 0, 1.0, 2.0) * jnp.where(slot_columns == 0, 1.0, 2.0)
            weight = weight * (-1.0 / (4 * grid * grid))
            return wave_rows, wave_columns, film, (1.0 - film) / safe, weight

        @pl.when(core == 1)
        def _():
            wave_rows, wave_columns, _, in_plane, weight = parts(row_odd, column_odd)
            tensors[0, pl.ds(at, 64), :] = in_plane * wave_columns * wave_columns * weight
            mixed = in_plane * wave_columns * wave_rows * weight
            sign = jnp.where((row_odd == column_odd) == (zh == 0), -1.0, 1.0)
            tensors[2, pl.ds(at, 64), :] = jnp.where((slot_rows == 0) | (slot_columns == 0), 0.0, mixed * sign)
            wave_rows, wave_columns, _, in_plane, weight = parts(1 - row_odd, 1 - column_odd)
            tensors[1, pl.ds(at, 64), :] = in_plane * wave_rows * wave_rows * weight

        @pl.when(core == 0)
        def _():
            _, _, film, _, weight = parts(row_odd, column_odd)
            tensors[0, pl.ds(at, 64), :] = film * weight

        return carry

    lax.fori_loop(0, grid // 64, fill, 0)

    for load in loads[3:]:
        load.wait()
    for k in range(4):
        links[0, k] = wide_links[k, pl.ds(pl.multiple_of(top + core * strip, 8), strip), :]
    current[0, :, 8 : 8 + strip, :] = base[0]
    probe[0] = base[0]

    own_lines = pl.ds(pl.multiple_of(number * strip, strip), strip)

    def to_unit(plane, r):
        kind, slot = (1, plane) if plane < 2 else (0, 0)
        target = (rest + r) % rest_count
        return remote(
            send.at[plane, target // multi], land.at[slot, own_lines, :],
            send_sems.at[plane, r], land_sems.at[slot, number], at_place(kind, target),
        )

    def landed(slot, index):
        return remote(
            send.at[slot, 0], land.at[slot, pl.ds(index * strip, strip), :],
            send_sems.at[slot, 0], land_sems.at[slot, index], owner(index),
        )

    def to_owner(plane, k):
        slot = plane if plane < 2 else 0
        index = (number + k) % space
        return remote(
            back.at[slot, pl.ds(index * strip, strip), :], got.at[plane, rest],
            back_sems.at[slot, k], got_sems.at[plane, rest], owner(index),
        )

    def gotten(plane, r):
        kind, slot = (1, plane) if plane < 2 else (0, 0)
        return remote(
            back.at[slot, pl.ds(0, strip), :], got.at[plane, r],
            back_sems.at[slot, 0], got_sems.at[plane, r], at_place(kind, r),
        )

    def each(first, last, action):
        def one(k, carry):
            action(k)
            return carry

        lax.fori_loop(first, last, one, 0)

    def push(plane):
        each(1, space, lambda k: to_owner(plane, k).start())
        got[plane, rest] = back[plane if plane < 2 else 0, own_lines, :]

    def transform(kind, passes):
        planes = [(row_odd, column_odd), (1 - row_odd, 1 - column_odd)] if kind == 1 else [(row_odd, column_odd)]
        columns = pl.ds(pl.multiple_of(share * width, width), width)
        for n, (_, odd) in enumerate(planes):
            each(1, space, lambda k: landed(n, (number + k) % space).wait_recv())
            spectrum = product(
                passes, split(land[n]), (table_high[odd, :, columns], table_low[odd, :, columns])
            )
            put(passes, (plane_high, plane_low), n, spectrum)
        step = half

        def mix(i, carry):
            at = pl.multiple_of(i * step, step)
            lines = pl.ds(at, step)
            both = [
                product(
                    passes, (turned_high[odd, lines, :], turned_low[odd, lines, :]), (plane_high[n], plane_low[n])
                )
                for n, (odd, _) in enumerate(planes)
            ]
            if kind == 1:
                cross_term = tensors[2, lines, :]
                values = [
                    tensors[0, lines, :] * both[0] + cross_term * both[1],
                    cross_term * both[0] + tensors[1, lines, :] * both[1],
                ]
            else:
                values = [tensors[0, lines, :] * both[0]]
            for n, value in enumerate(values):
                put(passes, (mixed_high, mixed_low), (n, lines), value)
            return carry

        lax.fori_loop(0, grid // step, mix, 0)
        for n, (odd_rows, odd_columns) in enumerate(planes):
            film = product(
                passes, (table_high[odd_rows], table_low[odd_rows]), (mixed_high[n], mixed_low[n])
            )
            back[n] = product(
                passes, split(film), (turned_high[odd_columns, columns, :], turned_low[odd_columns, columns, :])
            )
            push(n if kind == 1 else 2)

    def unit_work(kind, passes):
        @pl.when(core == kind)
        def _():
            transform(kind, passes)

    def unit_end(kind):
        @pl.when(core == kind)
        def _():
            for plane in (0, 1) if kind == 1 else (2,):
                each(1, space, lambda k: to_owner(plane, k).wait_send())

    def elsewhere(plane, r, action):
        pl.when((core != (1 if plane < 2 else 0)) | (r != 0))(action)

    def evaluate(parity, passes, first):
        outward = remote(
            edge_out.at[0], edge_in.at[parity, 1], edge_sems.at[parity, 0], edge_sems.at[parity, 1],
            owner((number + space - 1) % space),
        )
        inward = remote(
            edge_out.at[1], edge_in.at[parity, 0], edge_sems.at[parity, 2], edge_sems.at[parity, 3],
            owner((number + 1) % space),
        )
        fold_passes = min(passes, 2)
        for c in range(3):
            if first:
                start_swaps[c].wait()
                base[1, c] = far_start[c]
                probe[1, c] = far_start[c]
                current[1, c, 8 : 8 + strip, :] = far_start[c]
            near, far = probe[0, c], probe[1, c]
            lines = pl.ds(2 * c * strip, 2 * strip)
            for p, value in enumerate((near + far, near - far)):
                put(fold_passes, (wide_high, wide_low), pl.ds((2 * c + p) * strip, strip), value)
            folded = product(fold_passes, (wide_high[lines, :], wide_low[lines, :]), (fold[...],))
            for p in range(2):
                for q in range(2):
                    which = 2 * (1 - p) + 1 - q if c == 1 else 2 * p + q
                    send[c, which] = folded[p * strip : (p + 1) * strip, q * half : (q + 1) * half]
            each(0, rest_count, lambda r: elsewhere(c, r, lambda: to_unit(c, r).start()))

            @pl.when(core == (1 if c < 2 else 0))
            def _():
                land[c if c < 2 else 0, own_lines, :] = send[c, unit]

        for t in range(2):
            for c in range(3):
                edge_out[0, 3 * t + c : 3 * t + c + 1, :] = current[t, c, 8:9, :]
                edge_out[1, 3 * t + c : 3 * t + c + 1, :] = current[t, c, 7 + strip : 8 + strip, :]
        outward.start()
        inward.start()
        if first:
            for copy in field_swaps[EARLY:]:
                copy.start()
            coupling_swap.start()
        unit_work(1, passes)
        unit_work(0, passes)
        for c in (2, 0, 1):
            each(0, rest_count, lambda r: elsewhere(c, r, lambda: gotten(c, (rest + r) % rest_count).wait_recv()))
            lines = pl.ds(2 * c * strip, 2 * strip)
            for p in range(2):
                for q in range(2):
                    source = 2 * (1 - p) + 1 - q if c == 1 else 2 * p + q
                    value = None
                    for k in range(multi):
                        piece = got[c, source * multi + k]
                        value = piece if value is None else value + piece
                    where = (pl.ds((2 * c + p) * strip, strip), pl.ds(q * half, half))
                    put(fold_passes, (wide_high, wide_low), where, value)
            unfolded = product(fold_passes, (wide_high[lines, :], wide_low[lines, :]), (unfold[...],))
            even, odd = unfolded[:strip], unfolded[strip:]
            for t, value in enumerate((even + odd, even - odd)):
                if first:
                    demag[0, t, c] = value
                    demag[1, t, c] = value
                elif parity == 0:
                    moved = demag[0, t, c] + value
                    demag[0, t, c] = moved
                    demag[1, t, c] = moved
                else:
                    demag[1, t, c] = demag[0, t, c] + value
        for c in range(3):
            each(0, rest_count, lambda r: elsewhere(c, r, lambda: to_unit(c, r).wait_send()))
        outward.wait()
        inward.wait()
        if first:
            for copy in [*field_swaps, coupling_swap]:
                copy.wait()
            make_links(far_links, HALO, HALO + strip, far_coupling)
            links[1] = far_links[:, HALO : HALO + strip, :]
        unit_end(1)
        unit_end(0)
        last = number == space - 1
        for t in range(2):
            for c in range(3):
                current[t, c, 7:8, :] = edge_in[parity, 0, 3 * t + c : 3 * t + c + 1, :]
                facing = current[1 - t, c, 7 + strip : 8 + strip, :]
                arrived = edge_in[parity, 1, 3 * t + c : 3 * t + c + 1, :]
                current[t, c, 8 + strip : 9 + strip, :] = jnp.where(last, facing, arrived)
        for t in range(2):
            applied = (wide_field.at[:, pl.ds(pl.multiple_of(top + core * strip, 8), strip), :], far_field)[t]
            for at in range(0, strip, 8):
                rows_here = slice(at, at + 8)
                weights = [links[t, n, rows_here, :] for n in range(4)]
                inside, total = exchange(lambda c, where: current[t, c, where : where + 8, :], weights, 8 + at)
                effective = [total[c] + demag[1, t, c, rows_here, :] + applied[c, rows_here, :] for c in range(3)]
                moved = torque_of(inside, effective)
                for c in range(3):
                    if parity == 0:
                        rate[t, c, rows_here, :] = moved[c]
                        probe[t, c, rows_here, :] = step_time * moved[c]
                    else:
                        change = 0.5 * step_time * (rate[t, c, rows_here, :] + moved[c])
                        probe[t, c, rows_here, :] = change
                        base[t, c, rows_here, :] = base[t, c, rows_here, :] + change
        if parity == 0:
            current[:, :, 8 : 8 + strip, :] = base[...] + probe[...]
        else:
            current[:, :, 8 : 8 + strip, :] = base[...]

    evaluate(0, 3, True)

    def fine_step(i, carry):
        evaluate(1, PASSES, False)
        evaluate(0, PASSES, False)
        return carry

    lax.fori_loop(1, FINE, fine_step, 0)
    evaluate(1, PASSES, False)

    direct = core == zh
    away = {"core": zh, "zh": 1 - zh, "rest": mirror}
    beside = {"core": 1 - core}

    def carry_jump(t, where):
        return remote(base.at[t], jumps_in.at[core], jump_sends.at[t], jump_recvs.at[core], where)

    def await_jump(part):
        remote(base.at[0], jumps_in.at[part], jump_sends.at[0], jump_recvs.at[part], away).wait_recv()

    far, near = carry_jump(1, away), carry_jump(0, beside)
    far.start()

    @pl.when(jnp.logical_not(direct))
    def _():
        near.start()

    @pl.when(core == 0)
    def _():
        coarse_end[...] = state[1, :, top : top + rows, :]

    @pl.when(core == 1)
    def _():
        coarse_step(1)
        coarse_end[...] = state[0, :, top : top + rows, :]

    @pl.when(jnp.logical_not(direct))
    def _():
        await_jump(0)
        await_jump(1)

    @pl.when(direct)
    def _():
        jumps_in[core] = base[0]
        await_jump(1 - core)

    outer = jnp.where(first_block, 0, 1)
    inner = jnp.where(last_block, 1, 0)
    outgoing = [
        remote(source, target, chain_sends.at[n], chain_recvs.at[sem], in_slice(slice_number + 1, where))
        for n, (source, target, sem, where) in enumerate((
            (out, arrived.at[:, pl.ds(8, rows), :], 2, place),
            (last_out.at[0], last_in.at[outer], outer, outward_place),
            (last_out.at[1], last_in.at[inner], inner, inward_place),
        ))
    ]
    arrivals = [
        remote(source, target, chain_sends.at[0], chain_recvs.at[sem], in_slice(slice_number - 1, place))
        for source, target, sem in (
            (out, arrived.at[:, pl.ds(8, rows), :], 2),
            (last_out.at[0], last_in.at[0], 0),
            (last_out.at[1], last_in.at[1], 1),
        )
    ]

    @pl.when(slice_number == 0)
    def _():
        for c in range(3):
            for k in range(2):
                out[c, k * strip : (k + 1) * strip, :] = jumps_in[k, c]

    @pl.when(earlier)
    def _():
        for copy in arrivals:
            copy.wait_recv()
        for c in range(3):
            arrived[c, 7:8, :] = last_in[0, c : c + 1, :]
            arrived[c, 8 + rows : 9 + rows, :] = last_in[1, c : c + 1, :]
        for at in range(0, rows, 8):
            weights = [wide_links[n, top + at : top + at + 8, :] for n in range(4)]
            inside, total = exchange(lambda c, where: arrived[c, where : where + 8, :], weights, 8 + at)
            effective = [total[c] + wide_field[c, top + at : top + at + 8, :] for c in range(3)]
            effective[2] = effective[2] - inside[2]
            moved = torque_of(inside, effective)
            k, within = at // strip, at % strip
            for c in range(3):
                jump = jumps_in[k, c, within : within + 8, :] - coarse_end[c, at : at + 8, :]
                out[c, at : at + 8, :] = inside[c] + FINE * step_time * moved[c] + jump

    @pl.when(later)
    def _():
        for c in range(3):
            last_out[0, c : c + 1, :] = out[c, 0:1, :]
            last_out[1, c : c + 1, :] = out[c, rows - 1 : rows, :]
        for copy in outgoing:
            copy.start()
        for copy in outgoing:
            copy.wait_send()

    far.wait_send()

    @pl.when(jnp.logical_not(direct))
    def _():
        near.wait_send()

    @pl.when(jnp.logical_not(first_block))
    def _():
        to_outward.wait_send()

    to_inward.wait_send()

    @pl.when(zh == 1)
    def _():
        for c in range(3):
            for t in range(tiles // 2):
                low, high = slice(8 * t, 8 * t + 8), slice(rows - 8 - 8 * t, rows - 8 * t)
                upper, lower = flipped(out[c, high, :]), flipped(out[c, low, :])
                out[c, low, :] = upper
                out[c, high, :] = lower


def parareal(space, tm, start, field, coupling, tables):
    _, rows, grid = start.shape
    strip = rows // 2
    half = grid // 2
    rest_count = space // 2
    width = grid * 4 // rest_count
    f32, bf16 = jnp.float32, jnp.bfloat16
    operands = [start, field, coupling, *tables]
    return pl.pallas_call(
        functools.partial(parareal_kernel, space, tm),
        out_shape=jax.ShapeDtypeStruct((3, rows, grid), f32),
        in_specs=[pl.BlockSpec(memory_space=pl.ANY)] * TABLES,
        out_specs=pl.BlockSpec(memory_space=pltpu.VMEM),
        scratch_shapes=[
            *(pltpu.VMEM(operand.shape, operand.dtype) for operand in operands),
            pltpu.SemaphoreType.DMA((TABLES,)),
            pltpu.VMEM((2, 3, rows + 4 * HALO, grid), f32),
            pltpu.VMEM((3, rows + 4 * HALO, grid), f32),
            pltpu.VMEM((rows + 4 * HALO, grid), f32),
            pltpu.VMEM((4, rows + 4 * HALO, grid), f32),
            pltpu.VMEM((2, 7, HALO, grid), f32),
            pltpu.VMEM((2, 7, HALO, grid), f32),
            pltpu.VMEM((3, strip, grid), f32),
            pltpu.VMEM((3, rows, grid), f32),
            pltpu.VMEM((2, 3, strip + 16, grid), f32),
            pltpu.VMEM((2, 3, strip, grid), f32),
            pltpu.VMEM((2, 3, strip, grid), f32),
            pltpu.VMEM((2, 3, strip, grid), f32),
            pltpu.VMEM((2, 2, 3, strip, grid), f32),
            pltpu.VMEM((3, strip, grid), f32),
            pltpu.VMEM((3, strip, grid), f32),
            pltpu.VMEM((strip + 16, grid), f32),
            pltpu.VMEM((2, 4, strip, grid), f32),
            pltpu.VMEM((4, strip + 16, grid), f32),
            pltpu.VMEM((3, grid, width), f32),
            pltpu.VMEM((2, 8, grid), f32),
            pltpu.VMEM((2, 2, 8, grid), f32),
            pltpu.VMEM((6 * strip, grid), bf16),
            pltpu.VMEM((6 * strip, grid), bf16),
            pltpu.VMEM((3, 4, strip, half), f32),
            pltpu.VMEM((2, half, half), f32),
            pltpu.VMEM((2, half, half), f32),
            pltpu.VMEM((3, rest_count, strip, half), f32),
            pltpu.VMEM((2, half, width), bf16),
            pltpu.VMEM((2, half, width), bf16),
            pltpu.VMEM((2, grid, width), bf16),
            pltpu.VMEM((2, grid, width), bf16),
            pltpu.VMEM((2, 3, strip, grid), f32),
            pltpu.VMEM((3, rows + 16, grid), f32),
            pltpu.VMEM((2, 8, grid), f32),
            pltpu.VMEM((2, 8, grid), f32),
            pltpu.SemaphoreType.DMA((2, 2)),
            pltpu.SemaphoreType.DMA((2, 7)),
            pltpu.SemaphoreType.DMA((2, 4)),
            pltpu.SemaphoreType.DMA((3, rest_count)),
            pltpu.SemaphoreType.DMA((2, space)),
            pltpu.SemaphoreType.DMA((2, space)),
            pltpu.SemaphoreType.DMA((3, rest_count)),
            pltpu.SemaphoreType.DMA((2,)),
            pltpu.SemaphoreType.DMA((2,)),
            pltpu.SemaphoreType.DMA((3,)),
            pltpu.SemaphoreType.DMA((3,)),
        ],
        compiler_params=pltpu.CompilerParams(
            collective_id=0, has_side_effects=True, vmem_limit_bytes=VMEM_LIMIT
        ),
    )(*operands)


def make_shards(tm, space):
    def shards(initial_state, applied_field, coupling):
        grid = initial_state.shape[2]
        table, fold = sector_tables(grid)
        start = jnp.transpose(initial_state, (1, 0, 2))
        field = jnp.transpose(applied_field, (1, 0, 2))
        tables = [*halves(table), *halves(np.ascontiguousarray(np.transpose(table, (0, 2, 1))))]
        tables += [fold.astype(jnp.bfloat16), np.ascontiguousarray(fold.T).astype(jnp.bfloat16)]
        end = parareal(space, tm, start, field, coupling, tables)
        return jnp.transpose(end, (1, 0, 2))[None]

    return shards


def solution(mesh):
    tm, space = mesh.shape["tm"], mesh.shape["space"]
    finer = Mesh(mesh.devices.reshape(tm // 2, 2, 2, space // 2), EVERY)
    rows = ("zh", "rest")
    return jax.shard_map(
        make_shards(tm, space),
        mesh=finer,
        in_specs=(P(rows, None, None), P(rows, None, None), P(rows, None)),
        out_specs=P(("x", "core"), rows, None, None),
        check_vma=False,
    )
```

```python
import functools
import math

import jax
import jax.numpy as jnp
import numpy as np
from jax import lax
from jax.experimental import pallas as pl
from jax.experimental.pallas import tpu as pltpu
from jax.sharding import Mesh, PartitionSpec as P

FINE = 2
step_time = 0.06
damping = 0.02
stiffness = 0.25
thickness = 8.0
PASSES = 1

EVERY = ("x", "core", "zh", "rest")


def sector_tables(grid):
    half = grid // 2
    place = 2 * np.arange(half) - (grid - 1)
    wave = np.arange(grid)
    odd_wave = np.where(wave == 0, grid, wave)
    turn = 4 * grid

    def angle(k):
        return 2.0 * np.pi / turn * ((place[:, None] * k[None, :]) % turn)

    table = np.stack([np.cos(angle(wave)), np.sin(angle(odd_wave))]).astype(np.float32)
    fold = np.zeros((grid, grid), np.float32)
    for i in range(half):
        fold[i, i] = fold[grid - 1 - i, i] = fold[i, half + i] = 1.0
        fold[grid - 1 - i, half + i] = -1.0
    return table, fold


def halves(table):
    high = table.astype(jnp.bfloat16)
    return [high, (table - high.astype(np.float32)).astype(jnp.bfloat16)]


def split(value):
    high = value.astype(jnp.bfloat16)
    return high, (value - high.astype(jnp.float32)).astype(jnp.bfloat16)


def cross_of(a, b):
    return [a[1] * b[2] - a[2] * b[1], a[2] * b[0] - a[0] * b[2], a[0] * b[1] - a[1] * b[0]]


def product(passes, left, right):
    def one(a, b):
        return jnp.dot(a, b, preferred_element_type=jnp.float32)

    value = one(left[0], right[0])
    if passes > 1:
        value = value + one(left[1], right[0])
    if passes > 2:
        value = value + one(left[0], right[1])
    return value


def put(passes, pair, where, value):
    high, low = split(value)
    pair[0][where] = high
    if passes > 1:
        pair[1][where] = low


VMEM_LIMIT = 66_600_000
HALO = 8
EARLY = 2
TABLES = 9


def parareal_kernel(
    space, tm,
    *refs,
):
    sources, out, rest_refs = refs[:TABLES], refs[TABLES], refs[TABLES + 1 :]
    copies_in, rest_refs = rest_refs[: TABLES + 1], rest_refs[TABLES + 1 :]
    (
        start_in, field_in, coupling_in, table_high, table_low, turned_high, turned_low, fold, unfold, table_sems,
    ) = copies_in
    (
        state, wide_field, wide_coupling, wide_links, halo_out, halo_in, theirs, coarse_end,
        current, rate, base, probe, demag, far_start, far_field, far_coupling, links, far_links, tensors,
        edge_out, edge_in, wide_high, wide_low, send, land, back, got,
        plane_high, plane_low, mixed_high, mixed_low,
        jumps_in, arrived, last_out, last_in,
        halo_sems, swap_sems, edge_sems, send_sems, land_sems, back_sems, got_sems,
        jump_sends, jump_recvs, chain_sends, chain_recvs,
    ) = rest_refs
    loads = [
        pltpu.make_async_copy(source, target, table_sems.at[n])
        for n, (source, target) in enumerate(zip(sources, copies_in[:TABLES]))
    ]
    for load in loads:
        load.start()
    _, rows, grid = start_in.shape
    strip = rows // 2
    rest_count = space // 2
    half = grid // 2
    multi = rest_count // 4
    width = grid // multi
    core, zh, rest = lax.axis_index("core"), lax.axis_index("zh"), lax.axis_index("rest")
    axis_x = lax.axis_index("x")
    slice_number = axis_x * 2 + core
    place = zh * rest_count + rest
    order = jnp.where(zh == 0, rest, rest_count - 1 - rest)
    number = 2 * order + core
    unit = rest // multi
    share = rest % multi
    row_odd, column_odd = unit // 2, unit % 2
    outward_place = jnp.where(zh == 0, place + space - 1, place + 1) % space
    inward_place = jnp.where(zh == 0, place + 1, place + space - 1) % space
    first_block, last_block = order == 0, order == rest_count - 1
    mirror = rest_count - 1 - rest

    def at_place(core_index, rest_index):
        return {"core": core_index, "rest": rest_index}

    def owner(index):
        spot = index // 2
        return at_place(index % 2, jnp.where(zh == 0, spot, rest_count - 1 - spot))

    def block_at(where):
        return {"zh": where // rest_count, "rest": where % rest_count}

    def in_slice(which, where):
        return {
            "x": which // 2, "core": which % 2, "zh": where // rest_count, "rest": where % rest_count,
        }

    def remote(source, target, send_sem, recv_sem, where):
        return pltpu.make_async_remote_copy(
            src_ref=source, dst_ref=target, send_sem=send_sem, recv_sem=recv_sem,
            device_id=where, device_id_type=pl.DeviceIdType.MESH,
        )

    barrier = pltpu.get_barrier_semaphore()
    later, earlier = slice_number < tm - 1, slice_number > 0

    def greet(where):
        pl.semaphore_signal(barrier, inc=1, device_id=where, device_id_type=pl.DeviceIdType.MESH)

    def greet_group(k, carry):
        greet(owner((number + k) % space))
        return carry

    lax.fori_loop(1, space, greet_group, 0)
    for k in range(2):
        greet({"core": k, "zh": 1 - zh, "rest": mirror})

    @pl.when(later)
    def _():
        for where in (outward_place, place, inward_place):
            greet(in_slice(slice_number + 1, where))

    @pl.when(earlier)
    def _():
        for where in (outward_place, place, inward_place):
            greet(in_slice(slice_number - 1, where))

    core_rows = pl.ds(pl.multiple_of(2 * HALO + core * strip, 8), strip)
    top = 2 * HALO
    tiles = rows // 8
    sublane = lax.broadcasted_iota(jnp.int32, (8, grid), 0)

    def flipped(value):
        for k in (1, 2, 4):
            value = jnp.where(
                sublane // k % 2 == 1, pltpu.roll(value, k, 0), pltpu.roll(value, 8 - k, 0)
            )
        return value

    def natural(c, at):
        if c < 3:
            return start_in[c, at : at + 8, :]
        return field_in[c - 3, at : at + 8, :] if c < 6 else coupling_in[at : at + 8, :]

    def keep(c, at, value):
        lines = slice(top + at, top + at + 8)
        if c < 3:
            state[0, c, lines, :] = value
        elif c < 6:
            wide_field[c - 3, lines, :] = value
        else:
            wide_coupling[lines, :] = value

    for load in loads[:3]:
        load.wait()

    @pl.when(zh == 0)
    def _():
        for c in range(7):
            for t in range(tiles):
                keep(c, 8 * t, natural(c, 8 * t))
            halo_out[0, c] = natural(c, 0)
            halo_out[1, c] = natural(c, rows - 8)

    @pl.when(zh == 1)
    def _():
        for c in range(7):
            for t in range(tiles):
                value = flipped(natural(c, rows - 8 - 8 * t))
                keep(c, 8 * t, value)
                if t == 0:
                    halo_out[0, c] = value
                if t == tiles - 1:
                    halo_out[1, c] = value

    pl.semaphore_wait(barrier, space + 1 + jnp.where(later, 3, 0) + jnp.where(earlier, 3, 0))

    to_outward = remote(
        halo_out.at[0], halo_in.at[1], halo_sems.at[0, 0], halo_sems.at[1, 1], block_at(outward_place)
    )
    inner_slot = jnp.where(last_block, 1, 0)
    to_inward = remote(
        halo_out.at[1], halo_in.at[inner_slot],
        halo_sems.at[0, 1], halo_sems.at[1, inner_slot], block_at(inward_place),
    )

    def halo_arrival(slot):
        return remote(
            halo_out.at[0], halo_in.at[slot], halo_sems.at[0, 0], halo_sems.at[1, slot],
            block_at(inward_place),
        )

    @pl.when(jnp.logical_not(first_block))
    def _():
        to_outward.start()

    to_inward.start()

    partner = {"zh": 1 - zh, "rest": mirror}
    coupling_source = wide_coupling.at[pl.ds(pl.multiple_of(HALO + core * strip, 8), strip + 2 * HALO), :]
    start_swaps = [
        remote(theirs.at[c], far_start.at[c], swap_sems.at[0, c], swap_sems.at[1, c], partner) for c in range(3)
    ]
    field_swaps = [
        remote(
            wide_field.at[c, core_rows, :], far_field.at[c], swap_sems.at[0, 3 + c], swap_sems.at[1, 3 + c], partner
        )
        for c in range(3)
    ]
    coupling_swap = remote(coupling_source, far_coupling, swap_sems.at[0, 6], swap_sems.at[1, 6], partner)
    for copy in field_swaps[:EARLY]:
        copy.start()


    def set_halo(at, slot, lines):
        for r, line in enumerate(lines):
            state[0, :, at + r : at + r + 1, :] = halo_in[slot, 0:3, line : line + 1, :]
            wide_field[:, at + r : at + r + 1, :] = halo_in[slot, 3:6, line : line + 1, :]
            wide_coupling[at + r : at + r + 1, :] = halo_in[slot, 6, line : line + 1, :]

    def set_block(at, slot):
        state[0, :, at : at + HALO, :] = halo_in[slot, 0:3]
        wide_field[:, at : at + HALO, :] = halo_in[slot, 3:6]
        wide_coupling[at : at + HALO, :] = halo_in[slot, 6]

    @pl.when(first_block)
    def _():
        state[0, :, HALO : top, :] = jnp.zeros((3, HALO, grid), jnp.float32)
        wide_field[:, HALO : top, :] = jnp.zeros((3, HALO, grid), jnp.float32)
        wide_coupling[HALO : top, :] = jnp.zeros((HALO, grid), jnp.float32)

    @pl.when(jnp.logical_not(first_block))
    def _():
        halo_arrival(0).wait_recv()
        set_block(HALO, 0)

    halo_arrival(1).wait_recv()

    @pl.when(last_block)
    def _():
        set_halo(top + rows, 1, list(range(HALO))[::-1])

    @pl.when(jnp.logical_not(last_block))
    def _():
        set_block(top + rows, 1)

    for at in (HALO - 1, top + rows + HALO):
        edge = jnp.zeros((1, grid), jnp.float32)
        wide_coupling[at : at + 1, :] = edge
        for n in range(2):
            for c in range(3):
                state[n, c, at : at + 1, :] = edge

    def make_links(target, first, last, source):
        lane = lax.broadcasted_iota(jnp.int32, (8, grid), 1)
        for at in range(first, last, 8):
            centre = source[at : at + 8, :]
            own = stiffness * centre
            target[0, at : at + 8, :] = own * source[at - 1 : at + 7, :]
            target[1, at : at + 8, :] = own * source[at + 1 : at + 9, :]
            target[2, at : at + 8, :] = jnp.where(lane == 0, 0.0, own * pltpu.roll(centre, 1, 1))
            target[3, at : at + 8, :] = jnp.where(lane == grid - 1, 0.0, own * pltpu.roll(centre, grid - 1, 1))

    make_links(wide_links, HALO, top + rows + HALO, wide_coupling)

    def exchange(read, weights, at):
        total = []
        inside = []
        for c in range(3):
            m = read(c, at)
            value = weights[0] * (read(c, at - 1) - m)
            value = value + weights[1] * (read(c, at + 1) - m)
            value = value + weights[2] * (pltpu.roll(m, 1, 1) - m)
            total.append(value + weights[3] * (pltpu.roll(m, grid - 1, 1) - m))
            inside.append(m)
        return inside, total

    def torque_of(inside, effective):
        turned = cross_of(inside, effective)
        again = cross_of(inside, turned)
        return [-(turned[c] + damping * again[c]) * (1.0 / (1.0 + damping * damping)) for c in range(3)]

    def coarse_step(n):
        before, after = n % 2, (n + 1) % 2

        for at in range(HALO, top + rows + HALO, 8):
            weights = [wide_links[k, at : at + 8, :] for k in range(4)]
            inside, total = exchange(lambda c, where: state[before, c, where : where + 8, :], weights, at)
            effective = [total[c] + wide_field[c, at : at + 8, :] for c in range(3)]
            effective[2] = effective[2] - inside[2]
            moved = torque_of(inside, effective)
            for c in range(3):
                state[after, c, at : at + 8, :] = inside[c] + FINE * step_time * moved[c]

    def native(n):
        return state[n % 2, :, pl.ds(pl.multiple_of(top + core * strip, 8), strip), :]

    def step_pair(n, carry):
        coarse_step(0)
        coarse_step(1)
        return carry

    lax.fori_loop(0, axis_x, step_pair, 0)
    def send_start():
        for copy in start_swaps:
            copy.start()

    @pl.when(zh == 1)
    def _():
        theirs[...] = native(0)
        send_start()

    @pl.when(zh == 0)
    def _():
        base[0] = native(0)

    coarse_step(0)

    @pl.when(zh == 0)
    def _():
        theirs[...] = native(1)
        send_start()

    @pl.when(zh == 1)
    def _():
        base[0] = native(1)

    def fill(i, carry):
        at = pl.multiple_of(i * 64, 64)
        slot_rows = at + lax.broadcasted_iota(jnp.int32, (64, width), 0)
        slot_columns = share * width + lax.broadcasted_iota(jnp.int32, (64, width), 1)
        unit_length = 2.0 * math.pi / (2 * grid)

        def parts(odd_rows, odd_columns):
            rows = jnp.where((slot_rows == 0) & (odd_rows == 1), grid, slot_rows)
            columns = jnp.where((slot_columns == 0) & (odd_columns == 1), grid, slot_columns)
            wave_rows = unit_length * rows.astype(jnp.float32)
            wave_columns = unit_length * columns.astype(jnp.float32)
            squared = wave_rows * wave_rows + wave_columns * wave_columns
            nonzero = squared > 0.0
            safe = jnp.where(nonzero, squared, 1.0)
            scaled = jnp.sqrt(safe) * thickness
            film = jnp.where(nonzero, (1.0 - jnp.exp(-scaled)) / scaled, 1.0)
            weight = jnp.where(slot_rows == 0, 1.0, 2.0) * jnp.where(slot_columns == 0, 1.0, 2.0)
            weight = weight * (-1.0 / (4 * grid * grid))
            return wave_rows, wave_columns, film, (1.0 - film) / safe, weight

        @pl.when(core == 1)
        def _():
            wave_rows, wave_columns, _, in_plane, weight = parts(row_odd, column_odd)
            tensors[0, pl.ds(at, 64), :] = in_plane * wave_columns * wave_columns * weight
            mixed = in_plane * wave_columns * wave_rows * weight
            sign = jnp.where((row_odd == column_odd) == (zh == 0), -1.0, 1.0)
            tensors[2, pl.ds(at, 64), :] = jnp.where((slot_rows == 0) | (slot_columns == 0), 0.0, mixed * sign)
            wave_rows, wave_columns, _, in_plane, weight = parts(1 - row_odd, 1 - column_odd)
            tensors[1, pl.ds(at, 64), :] = in_plane * wave_rows * wave_rows * weight

        @pl.when(core == 0)
        def _():
            _, _, film, _, weight = parts(row_odd, column_odd)
            tensors[0, pl.ds(at, 64), :] = film * weight

        return carry

    lax.fori_loop(0, grid // 64, fill, 0)

    for load in loads[3:]:
        load.wait()
    for k in range(4):
        links[0, k] = wide_links[k, pl.ds(pl.multiple_of(top + core * strip, 8), strip), :]
    current[0, :, 8 : 8 + strip, :] = base[0]
    probe[0] = base[0]

    own_lines = pl.ds(pl.multiple_of(number * strip, strip), strip)

    def across(r):
        return (rest // 2 + r // 2) % (rest_count // 2) * 2 + (rest + r) % 2

    def to_unit(plane, r):
        kind, slot = (1, plane) if plane < 2 else (0, 0)
        target = across(r)
        return remote(
            send.at[plane, target // multi], land.at[slot, own_lines, :],
            send_sems.at[plane, r], land_sems.at[slot, number], at_place(kind, target),
        )

    def landed(slot, index):
        return remote(
            send.at[slot, 0], land.at[slot, pl.ds(index * strip, strip), :],
            send_sems.at[slot, 0], land_sems.at[slot, index], owner(index),
        )

    def to_owner(plane, k):
        slot = plane if plane < 2 else 0
        target = across(k // 2)
        spot = jnp.where(zh == 0, target, rest_count - 1 - target)
        index = 2 * spot + (core + k) % 2
        return remote(
            back.at[slot, pl.ds(index * strip, strip), :], got.at[plane, rest],
            back_sems.at[slot, k], got_sems.at[plane, rest], owner(index),
        )

    def gotten(plane, r):
        kind, slot = (1, plane) if plane < 2 else (0, 0)
        return remote(
            back.at[slot, pl.ds(0, strip), :], got.at[plane, r],
            back_sems.at[slot, 0], got_sems.at[plane, r], at_place(kind, r),
        )

    def each(first, last, action):
        def one(k, carry):
            action(k)
            return carry

        lax.fori_loop(first, last, one, 0)

    def push(plane):
        each(0, space - 1, lambda k: to_owner(plane, space - 1 - k).start())
        got[plane, rest] = back[plane if plane < 2 else 0, own_lines, :]

    def transform(kind, passes):
        planes = [(row_odd, column_odd), (1 - row_odd, 1 - column_odd)] if kind == 1 else [(row_odd, column_odd)]
        columns = pl.ds(pl.multiple_of(share * width, width), width)
        for n, (_, odd) in enumerate(planes):
            each(1, space, lambda k: landed(n, (number + k) % space).wait_recv())
            spectrum = product(
                passes, split(land[n]), (table_high[odd, :, columns], table_low[odd, :, columns])
            )
            put(passes, (plane_high, plane_low), n, spectrum)
        step = half

        def mix(i, carry):
            at = pl.multiple_of(i * step, step)
            lines = pl.ds(at, step)
            both = [
                product(
                    passes, (turned_high[odd, lines, :], turned_low[odd, lines, :]), (plane_high[n], plane_low[n])
                )
                for n, (odd, _) in enumerate(planes)
            ]
            if kind == 1:
                cross_term = tensors[2, lines, :]
                values = [
                    tensors[0, lines, :] * both[0] + cross_term * both[1],
                    cross_term * both[0] + tensors[1, lines, :] * both[1],
                ]
            else:
                values = [tensors[0, lines, :] * both[0]]
            for n, value in enumerate(values):
                put(passes, (mixed_high, mixed_low), (n, lines), value)
            return carry

        lax.fori_loop(0, grid // step, mix, 0)
        for n, (odd_rows, odd_columns) in enumerate(planes):
            film = product(
                passes, (table_high[odd_rows], table_low[odd_rows]), (mixed_high[n], mixed_low[n])
            )
            back[n] = product(
                passes, split(film), (turned_high[odd_columns, columns, :], turned_low[odd_columns, columns, :])
            )
            push(n if kind == 1 else 2)

    def unit_work(kind, passes):
        @pl.when(core == kind)
        def _():
            transform(kind, passes)

    def unit_end(kind):
        @pl.when(core == kind)
        def _():
            for plane in (0, 1) if kind == 1 else (2,):
                each(1, space, lambda k: to_owner(plane, k).wait_send())

    def elsewhere(plane, r, action):
        pl.when((core != (1 if plane < 2 else 0)) | (r != 0))(action)

    def evaluate(parity, passes, first, last_one=None):
        outward = remote(
            edge_out.at[0], edge_in.at[parity, 1], edge_sems.at[parity, 0], edge_sems.at[parity, 1],
            owner((number + space - 1) % space),
        )
        inward = remote(
            edge_out.at[1], edge_in.at[parity, 0], edge_sems.at[parity, 2], edge_sems.at[parity, 3],
            owner((number + 1) % space),
        )
        fold_passes = min(passes, 2)
        for c in range(3):
            if first:
                start_swaps[c].wait()
                base[1, c] = far_start[c]
                probe[1, c] = far_start[c]
                current[1, c, 8 : 8 + strip, :] = far_start[c]
            near, far = probe[0, c], probe[1, c]
            lines = pl.ds(2 * c * strip, 2 * strip)
            for p, value in enumerate((near + far, near - far)):
                put(fold_passes, (wide_high, wide_low), pl.ds((2 * c + p) * strip, strip), value)
            folded = product(fold_passes, (wide_high[lines, :], wide_low[lines, :]), (fold[...],))
            for p in range(2):
                for q in range(2):
                    which = 2 * (1 - p) + 1 - q if c == 1 else 2 * p + q
                    send[c, which] = folded[p * strip : (p + 1) * strip, q * half : (q + 1) * half]
            each(0, rest_count, lambda r: elsewhere(
                c, rest_count - 1 - r, lambda: to_unit(c, rest_count - 1 - r).start()
            ))

            @pl.when(core == (1 if c < 2 else 0))
            def _():
                land[c if c < 2 else 0, own_lines, :] = send[c, unit]

        for t in range(2):
            for c in range(3):
                edge_out[0, 3 * t + c : 3 * t + c + 1, :] = current[t, c, 8:9, :]
                edge_out[1, 3 * t + c : 3 * t + c + 1, :] = current[t, c, 7 + strip : 8 + strip, :]
        outward.start()
        inward.start()
        if first:
            for copy in field_swaps[EARLY:]:
                copy.start()
            coupling_swap.start()
        unit_work(1, passes)
        unit_work(0, passes)
        for c in (2, 0, 1):
            each(0, rest_count, lambda r: elsewhere(c, r, lambda: gotten(c, (rest + r) % rest_count).wait_recv()))
            lines = pl.ds(2 * c * strip, 2 * strip)
            for p in range(2):
                for q in range(2):
                    source = 2 * (1 - p) + 1 - q if c == 1 else 2 * p + q
                    value = None
                    for k in range(multi):
                        piece = got[c, source * multi + k]
                        value = piece if value is None else value + piece
                    where = (pl.ds((2 * c + p) * strip, strip), pl.ds(q * half, half))
                    put(fold_passes, (wide_high, wide_low), where, value)
            unfolded = product(fold_passes, (wide_high[lines, :], wide_low[lines, :]), (unfold[...],))
            even, odd = unfolded[:strip], unfolded[strip:]
            for t, value in enumerate((even + odd, even - odd)):
                if first:
                    demag[0, t, c] = value
                    demag[1, t, c] = value
                elif parity == 0:
                    moved = demag[0, t, c] + value
                    demag[0, t, c] = moved
                    demag[1, t, c] = moved
                else:
                    demag[1, t, c] = demag[0, t, c] + value
        for c in range(3):
            each(0, rest_count, lambda r: elsewhere(c, r, lambda: to_unit(c, r).wait_send()))
        outward.wait()
        inward.wait()
        if first:
            for copy in [*field_swaps, coupling_swap]:
                copy.wait()
            make_links(far_links, HALO, HALO + strip, far_coupling)
            links[1] = far_links[:, HALO : HALO + strip, :]
        unit_end(1)
        unit_end(0)
        last = number == space - 1
        for t in range(2):
            for c in range(3):
                current[t, c, 7:8, :] = edge_in[parity, 0, 3 * t + c : 3 * t + c + 1, :]
                facing = current[1 - t, c, 7 + strip : 8 + strip, :]
                arrived = edge_in[parity, 1, 3 * t + c : 3 * t + c + 1, :]
                current[t, c, 8 + strip : 9 + strip, :] = jnp.where(last, facing, arrived)
        for t in (1, 0):
            applied = (wide_field.at[:, pl.ds(pl.multiple_of(top + core * strip, 8), strip), :], far_field)[t]
            for at in range(0, strip, 8):
                rows_here = slice(at, at + 8)
                weights = [links[t, n, rows_here, :] for n in range(4)]
                inside, total = exchange(lambda c, where: current[t, c, where : where + 8, :], weights, 8 + at)
                effective = [total[c] + demag[1, t, c, rows_here, :] + applied[c, rows_here, :] for c in range(3)]
                moved = torque_of(inside, effective)
                for c in range(3):
                    if parity == 0:
                        rate[t, c, rows_here, :] = moved[c]
                        probe[t, c, rows_here, :] = step_time * moved[c]
                    else:
                        change = 0.5 * step_time * (rate[t, c, rows_here, :] + moved[c])
                        probe[t, c, rows_here, :] = change
                        base[t, c, rows_here, :] = base[t, c, rows_here, :] + change
            if t == 1 and last_one is not None:
                last_one()
        if parity == 0:
            current[:, :, 8 : 8 + strip, :] = base[...] + probe[...]
        else:
            current[:, :, 8 : 8 + strip, :] = base[...]

    evaluate(0, 3, True)

    def fine_step(i, carry):
        evaluate(1, PASSES, False)
        evaluate(0, PASSES, False)
        return carry

    lax.fori_loop(1, FINE, fine_step, 0)
    direct = core == zh
    away = {"core": zh, "zh": 1 - zh, "rest": mirror}
    beside = {"core": 1 - core}

    def carry_jump(t, where):
        return remote(base.at[t], jumps_in.at[core], jump_sends.at[t], jump_recvs.at[core], where)

    def await_jump(part):
        remote(base.at[0], jumps_in.at[part], jump_sends.at[0], jump_recvs.at[part], away).wait_recv()

    far, near = carry_jump(1, away), carry_jump(0, beside)
    evaluate(1, PASSES, False, far.start)

    @pl.when(jnp.logical_not(direct))
    def _():
        near.start()

    @pl.when(core == 0)
    def _():
        coarse_end[...] = state[1, :, top : top + rows, :]

    @pl.when(core == 1)
    def _():
        coarse_step(1)
        coarse_end[...] = state[0, :, top : top + rows, :]

    @pl.when(jnp.logical_not(direct))
    def _():
        await_jump(0)
        await_jump(1)

    @pl.when(direct)
    def _():
        jumps_in[core] = base[0]
        await_jump(1 - core)

    outer = jnp.where(first_block, 0, 1)
    inner = jnp.where(last_block, 1, 0)
    outgoing = [
        remote(source, target, chain_sends.at[n], chain_recvs.at[sem], in_slice(slice_number + 1, where))
        for n, (source, target, sem, where) in enumerate((
            (out, arrived.at[:, pl.ds(8, rows), :], 2, place),
            (last_out.at[0], last_in.at[outer], outer, outward_place),
            (last_out.at[1], last_in.at[inner], inner, inward_place),
        ))
    ]
    arrivals = [
        remote(source, target, chain_sends.at[0], chain_recvs.at[sem], in_slice(slice_number - 1, place))
        for source, target, sem in (
            (out, arrived.at[:, pl.ds(8, rows), :], 2),
            (last_out.at[0], last_in.at[0], 0),
            (last_out.at[1], last_in.at[1], 1),
        )
    ]

    def send_edges():
        @pl.when(later)
        def _():
            for c in range(3):
                last_out[0, c : c + 1, :] = out[c, 0:1, :]
                last_out[1, c : c + 1, :] = out[c, rows - 1 : rows, :]
            outgoing[1].start()
            outgoing[2].start()

    @pl.when(slice_number == 0)
    def _():
        for c in range(3):
            for k in range(2):
                out[c, k * strip : (k + 1) * strip, :] = jumps_in[k, c]
        send_edges()

    @pl.when(earlier)
    def _():
        for copy in arrivals:
            copy.wait_recv()
        for c in range(3):
            arrived[c, 7:8, :] = last_in[0, c : c + 1, :]
            arrived[c, 8 + rows : 9 + rows, :] = last_in[1, c : c + 1, :]

        def advance(at):
            weights = [wide_links[n, top + at : top + at + 8, :] for n in range(4)]
            inside, total = exchange(lambda c, where: arrived[c, where : where + 8, :], weights, 8 + at)
            effective = [total[c] + wide_field[c, top + at : top + at + 8, :] for c in range(3)]
            effective[2] = effective[2] - inside[2]
            moved = torque_of(inside, effective)
            k, within = at // strip, at % strip
            for c in range(3):
                jump = jumps_in[k, c, within : within + 8, :] - coarse_end[c, at : at + 8, :]
                out[c, at : at + 8, :] = inside[c] + FINE * step_time * moved[c] + jump

        advance(0)
        advance(rows - 8)
        send_edges()
        for at in range(8, rows - 8, 8):
            advance(at)

    @pl.when(later)
    def _():
        outgoing[0].start()
        for copy in outgoing:
            copy.wait_send()

    far.wait_send()

    @pl.when(jnp.logical_not(direct))
    def _():
        near.wait_send()

    @pl.when(jnp.logical_not(first_block))
    def _():
        to_outward.wait_send()

    to_inward.wait_send()

    @pl.when(zh == 1)
    def _():
        for c in range(3):
            for t in range(tiles // 2):
                low, high = slice(8 * t, 8 * t + 8), slice(rows - 8 - 8 * t, rows - 8 * t)
                upper, lower = flipped(out[c, high, :]), flipped(out[c, low, :])
                out[c, low, :] = upper
                out[c, high, :] = lower


def parareal(space, tm, start, field, coupling, tables):
    _, rows, grid = start.shape
    strip = rows // 2
    half = grid // 2
    rest_count = space // 2
    width = grid * 4 // rest_count
    f32, bf16 = jnp.float32, jnp.bfloat16
    operands = [start, field, coupling, *tables]
    return pl.pallas_call(
        functools.partial(parareal_kernel, space, tm),
        out_shape=jax.ShapeDtypeStruct((3, rows, grid), f32),
        in_specs=[pl.BlockSpec(memory_space=pl.ANY)] * TABLES,
        out_specs=pl.BlockSpec(memory_space=pltpu.VMEM),
        scratch_shapes=[
            *(pltpu.VMEM(operand.shape, operand.dtype) for operand in operands),
            pltpu.SemaphoreType.DMA((TABLES,)),
            pltpu.VMEM((2, 3, rows + 4 * HALO, grid), f32),
            pltpu.VMEM((3, rows + 4 * HALO, grid), f32),
            pltpu.VMEM((rows + 4 * HALO, grid), f32),
            pltpu.VMEM((4, rows + 4 * HALO, grid), f32),
            pltpu.VMEM((2, 7, HALO, grid), f32),
            pltpu.VMEM((2, 7, HALO, grid), f32),
            pltpu.VMEM((3, strip, grid), f32),
            pltpu.VMEM((3, rows, grid), f32),
            pltpu.VMEM((2, 3, strip + 16, grid), f32),
            pltpu.VMEM((2, 3, strip, grid), f32),
            pltpu.VMEM((2, 3, strip, grid), f32),
            pltpu.VMEM((2, 3, strip, grid), f32),
            pltpu.VMEM((2, 2, 3, strip, grid), f32),
            pltpu.VMEM((3, strip, grid), f32),
            pltpu.VMEM((3, strip, grid), f32),
            pltpu.VMEM((strip + 16, grid), f32),
            pltpu.VMEM((2, 4, strip, grid), f32),
            pltpu.VMEM((4, strip + 16, grid), f32),
            pltpu.VMEM((3, grid, width), f32),
            pltpu.VMEM((2, 8, grid), f32),
            pltpu.VMEM((2, 2, 8, grid), f32),
            pltpu.VMEM((6 * strip, grid), bf16),
            pltpu.VMEM((6 * strip, grid), bf16),
            pltpu.VMEM((3, 4, strip, half), f32),
            pltpu.VMEM((2, half, half), f32),
            pltpu.VMEM((2, half, half), f32),
            pltpu.VMEM((3, rest_count, strip, half), f32),
            pltpu.VMEM((2, half, width), bf16),
            pltpu.VMEM((2, half, width), bf16),
            pltpu.VMEM((2, grid, width), bf16),
            pltpu.VMEM((2, grid, width), bf16),
            pltpu.VMEM((2, 3, strip, grid), f32),
            pltpu.VMEM((3, rows + 16, grid), f32),
            pltpu.VMEM((2, 8, grid), f32),
            pltpu.VMEM((2, 8, grid), f32),
            pltpu.SemaphoreType.DMA((2, 2)),
            pltpu.SemaphoreType.DMA((2, 7)),
            pltpu.SemaphoreType.DMA((2, 4)),
            pltpu.SemaphoreType.DMA((3, rest_count)),
            pltpu.SemaphoreType.DMA((2, space)),
            pltpu.SemaphoreType.DMA((2, space)),
            pltpu.SemaphoreType.DMA((3, rest_count)),
            pltpu.SemaphoreType.DMA((2,)),
            pltpu.SemaphoreType.DMA((2,)),
            pltpu.SemaphoreType.DMA((3,)),
            pltpu.SemaphoreType.DMA((3,)),
        ],
        compiler_params=pltpu.CompilerParams(
            collective_id=0, has_side_effects=True, vmem_limit_bytes=VMEM_LIMIT
        ),
    )(*operands)


def make_shards(tm, space):
    def shards(initial_state, applied_field, coupling):
        grid = initial_state.shape[2]
        table, fold = sector_tables(grid)
        start = jnp.transpose(initial_state, (1, 0, 2))
        field = jnp.transpose(applied_field, (1, 0, 2))
        tables = [*halves(table), *halves(np.ascontiguousarray(np.transpose(table, (0, 2, 1))))]
        tables += [fold.astype(jnp.bfloat16), np.ascontiguousarray(fold.T).astype(jnp.bfloat16)]
        end = parareal(space, tm, start, field, coupling, tables)
        return jnp.transpose(end, (1, 0, 2))[None]

    return shards


def solution(mesh):
    tm, space = mesh.shape["tm"], mesh.shape["space"]
    finer = Mesh(mesh.devices.reshape(tm // 2, 2, 2, space // 2), EVERY)
    rows = ("zh", "rest")
    return jax.shard_map(
        make_shards(tm, space),
        mesh=finer,
        in_specs=(P(rows, None, None), P(rows, None, None), P(rows, None)),
        out_specs=P(("x", "core"), rows, None, None),
        check_vma=False,
    )
```

```python
import functools
import math

import jax
import jax.numpy as jnp
import numpy as np
from jax import lax
from jax.experimental import pallas as pl
from jax.experimental.pallas import tpu as pltpu
from jax.sharding import Mesh, PartitionSpec as P

FINE = 2
step_time = 0.06
damping = 0.02
stiffness = 0.25
thickness = 8.0
PASSES = 1

EVERY = ("x", "core", "zh", "rest")


def sector_tables(grid):
    half = grid // 2
    place = 2 * np.arange(half) - (grid - 1)
    wave = np.arange(grid)
    odd_wave = np.where(wave == 0, grid, wave)
    turn = 4 * grid

    def angle(k):
        return 2.0 * np.pi / turn * ((place[:, None] * k[None, :]) % turn)

    table = np.stack([np.cos(angle(wave)), np.sin(angle(odd_wave))]).astype(np.float32)
    fold = np.zeros((grid, grid), np.float32)
    for i in range(half):
        fold[i, i] = fold[grid - 1 - i, i] = fold[i, half + i] = 1.0
        fold[grid - 1 - i, half + i] = -1.0
    return table, fold


def halves(table):
    high = table.astype(jnp.bfloat16)
    return [high, (table - high.astype(np.float32)).astype(jnp.bfloat16)]


def split(value):
    high = value.astype(jnp.bfloat16)
    return high, (value - high.astype(jnp.float32)).astype(jnp.bfloat16)


def cross_of(a, b):
    return [a[1] * b[2] - a[2] * b[1], a[2] * b[0] - a[0] * b[2], a[0] * b[1] - a[1] * b[0]]


def product(passes, left, right):
    def one(a, b):
        return jnp.dot(a, b, preferred_element_type=jnp.float32)

    value = one(left[0], right[0])
    if passes > 1:
        value = value + one(left[1], right[0])
    if passes > 2:
        value = value + one(left[0], right[1])
    return value


def put(passes, pair, where, value):
    high, low = split(value)
    pair[0][where] = high
    if passes > 1:
        pair[1][where] = low


VMEM_LIMIT = 66_600_000
HALO = 8
EARLY = 2
TABLES = 9


def parareal_kernel(
    space, tm,
    *refs,
):
    sources, out, rest_refs = refs[:TABLES], refs[TABLES], refs[TABLES + 1 :]
    copies_in, rest_refs = rest_refs[: TABLES + 1], rest_refs[TABLES + 1 :]
    (
        start_in, field_in, coupling_in, table_high, table_low, turned_high, turned_low, fold, unfold, table_sems,
    ) = copies_in
    (
        state, wide_field, wide_coupling, wide_links, halo_out, halo_in, theirs, coarse_end,
        current, rate, base, probe, demag, far_start, far_field, far_coupling, links, far_links, tensors,
        edge_out, edge_in, wide_high, wide_low, send, land, back, got,
        plane_high, plane_low, mixed_high, mixed_low,
        jumps_in, arrived, last_out, last_in,
        halo_sems, swap_sems, edge_sems, send_sems, land_sems, back_sems, got_sems,
        jump_sends, jump_recvs, chain_sends, chain_recvs,
    ) = rest_refs
    loads = [
        pltpu.make_async_copy(source, target, table_sems.at[n])
        for n, (source, target) in enumerate(zip(sources, copies_in[:TABLES]))
    ]
    for load in loads:
        load.start()
    _, rows, grid = start_in.shape
    strip = rows // 2
    rest_count = space // 2
    half = grid // 2
    multi = rest_count // 4
    width = grid // multi
    core, zh, rest = lax.axis_index("core"), lax.axis_index("zh"), lax.axis_index("rest")
    axis_x = lax.axis_index("x")
    slice_number = axis_x * 2 + core
    place = zh * rest_count + rest
    order = jnp.where(zh == 0, rest, rest_count - 1 - rest)
    number = 2 * order + core
    unit = rest // multi
    share = rest % multi
    row_odd, column_odd = unit // 2, unit % 2
    outward_place = jnp.where(zh == 0, place + space - 1, place + 1) % space
    inward_place = jnp.where(zh == 0, place + 1, place + space - 1) % space
    first_block, last_block = order == 0, order == rest_count - 1
    mirror = rest_count - 1 - rest

    def at_place(core_index, rest_index):
        return {"core": core_index, "rest": rest_index}

    def owner(index):
        spot = index // 2
        return at_place(index % 2, jnp.where(zh == 0, spot, rest_count - 1 - spot))

    def block_at(where):
        return {"zh": where // rest_count, "rest": where % rest_count}

    def in_slice(which, where):
        return {
            "x": which // 2, "core": which % 2, "zh": where // rest_count, "rest": where % rest_count,
        }

    def remote(source, target, send_sem, recv_sem, where):
        return pltpu.make_async_remote_copy(
            src_ref=source, dst_ref=target, send_sem=send_sem, recv_sem=recv_sem,
            device_id=where, device_id_type=pl.DeviceIdType.MESH,
        )

    barrier = pltpu.get_barrier_semaphore()
    later, earlier = slice_number < tm - 1, slice_number > 0

    def greet(where):
        pl.semaphore_signal(barrier, inc=1, device_id=where, device_id_type=pl.DeviceIdType.MESH)

    def greet_group(k, carry):
        greet(owner((number + k) % space))
        return carry

    lax.fori_loop(1, space, greet_group, 0)
    for k in range(2):
        greet({"core": k, "zh": 1 - zh, "rest": mirror})

    @pl.when(later)
    def _():
        for where in (outward_place, place, inward_place):
            greet(in_slice(slice_number + 1, where))

    @pl.when(earlier)
    def _():
        for where in (outward_place, place, inward_place):
            greet(in_slice(slice_number - 1, where))

    core_rows = pl.ds(pl.multiple_of(2 * HALO + core * strip, 8), strip)
    top = 2 * HALO
    tiles = rows // 8
    sublane = lax.broadcasted_iota(jnp.int32, (8, grid), 0)

    def flipped(value):
        for k in (1, 2, 4):
            value = jnp.where(
                sublane // k % 2 == 1, pltpu.roll(value, k, 0), pltpu.roll(value, 8 - k, 0)
            )
        return value

    def natural(c, at):
        if c < 3:
            return start_in[c, at : at + 8, :]
        return field_in[c - 3, at : at + 8, :] if c < 6 else coupling_in[at : at + 8, :]

    def keep(c, at, value):
        lines = slice(top + at, top + at + 8)
        if c < 3:
            state[0, c, lines, :] = value
        elif c < 6:
            wide_field[c - 3, lines, :] = value
        else:
            wide_coupling[lines, :] = value

    for load in loads[:3]:
        load.wait()

    @pl.when(zh == 0)
    def _():
        for c in range(7):
            for t in range(tiles):
                keep(c, 8 * t, natural(c, 8 * t))
            halo_out[0, tm * c : tm * c + tm, :] = natural(c, 0)[:tm]
            halo_out[1, tm * c : tm * c + tm, :] = natural(c, rows - 8)[8 - tm :]

    @pl.when(zh == 1)
    def _():
        for c in range(7):
            for t in range(tiles):
                value = flipped(natural(c, rows - 8 - 8 * t))
                keep(c, 8 * t, value)
                if t == 0:
                    halo_out[0, tm * c : tm * c + tm, :] = value[:tm]
                if t == tiles - 1:
                    halo_out[1, tm * c : tm * c + tm, :] = value[8 - tm :]

    pl.semaphore_wait(barrier, space + 1 + jnp.where(later, 3, 0) + jnp.where(earlier, 3, 0))

    to_outward = remote(
        halo_out.at[0], halo_in.at[1], halo_sems.at[0, 0], halo_sems.at[1, 1], block_at(outward_place)
    )
    inner_slot = jnp.where(last_block, 1, 0)
    to_inward = remote(
        halo_out.at[1], halo_in.at[inner_slot],
        halo_sems.at[0, 1], halo_sems.at[1, inner_slot], block_at(inward_place),
    )

    def halo_arrival(slot):
        return remote(
            halo_out.at[0], halo_in.at[slot], halo_sems.at[0, 0], halo_sems.at[1, slot],
            block_at(inward_place),
        )

    @pl.when(jnp.logical_not(first_block))
    def _():
        to_outward.start()

    to_inward.start()

    partner = {"zh": 1 - zh, "rest": mirror}
    coupling_source = wide_coupling.at[pl.ds(pl.multiple_of(HALO + core * strip, 8), strip + 2 * HALO), :]
    start_swaps = [
        remote(theirs.at[c], far_start.at[c], swap_sems.at[0, c], swap_sems.at[1, c], partner) for c in range(3)
    ]
    field_swaps = [
        remote(
            wide_field.at[c, core_rows, :], far_field.at[c], swap_sems.at[0, 3 + c], swap_sems.at[1, 3 + c], partner
        )
        for c in range(3)
    ]
    coupling_swap = remote(coupling_source, far_coupling, swap_sems.at[0, 6], swap_sems.at[1, 6], partner)
    for copy in field_swaps[:EARLY]:
        copy.start()


    def set_halo(at, slot, backwards):
        for c in range(7):
            target = (state.at[0, c] if c < 3 else None, wide_field.at[c - 3] if 3 <= c < 6 else None, wide_coupling)[min(c // 3, 2)]
            if backwards:
                for r in range(tm):
                    line = tm * c + tm - 1 - r
                    target[at + r : at + r + 1, :] = halo_in[slot, line : line + 1, :]
            else:
                target[at : at + tm, :] = halo_in[slot, tm * c : tm * c + tm, :]

    @pl.when(first_block)
    def _():
        state[0, :, HALO : top, :] = jnp.zeros((3, HALO, grid), jnp.float32)
        wide_field[:, HALO : top, :] = jnp.zeros((3, HALO, grid), jnp.float32)
        wide_coupling[HALO : top, :] = jnp.zeros((HALO, grid), jnp.float32)

    @pl.when(jnp.logical_not(first_block))
    def _():
        halo_arrival(0).wait_recv()
        set_halo(top - tm, 0, False)

    halo_arrival(1).wait_recv()

    @pl.when(last_block)
    def _():
        set_halo(top + rows, 1, True)

    @pl.when(jnp.logical_not(last_block))
    def _():
        set_halo(top + rows, 1, False)

    for at in (HALO - 1, top + rows + HALO):
        edge = jnp.zeros((1, grid), jnp.float32)
        wide_coupling[at : at + 1, :] = edge
        for n in range(2):
            for c in range(3):
                state[n, c, at : at + 1, :] = edge

    def make_links(target, first, last, source):
        lane = lax.broadcasted_iota(jnp.int32, (8, grid), 1)
        for at in range(first, last, 8):
            centre = source[at : at + 8, :]
            own = stiffness * centre
            target[0, at : at + 8, :] = own * source[at - 1 : at + 7, :]
            target[1, at : at + 8, :] = own * source[at + 1 : at + 9, :]
            target[2, at : at + 8, :] = jnp.where(lane == 0, 0.0, own * pltpu.roll(centre, 1, 1))
            target[3, at : at + 8, :] = jnp.where(lane == grid - 1, 0.0, own * pltpu.roll(centre, grid - 1, 1))

    make_links(wide_links, HALO, top + rows + HALO, wide_coupling)

    def exchange(read, weights, at):
        total = []
        inside = []
        for c in range(3):
            m = read(c, at)
            value = weights[0] * (read(c, at - 1) - m)
            value = value + weights[1] * (read(c, at + 1) - m)
            value = value + weights[2] * (pltpu.roll(m, 1, 1) - m)
            total.append(value + weights[3] * (pltpu.roll(m, grid - 1, 1) - m))
            inside.append(m)
        return inside, total

    def torque_of(inside, effective):
        turned = cross_of(inside, effective)
        again = cross_of(inside, turned)
        return [-(turned[c] + damping * again[c]) * (1.0 / (1.0 + damping * damping)) for c in range(3)]

    def coarse_step(n):
        before, after = n % 2, (n + 1) % 2

        for at in range(HALO, top + rows + HALO, 8):
            weights = [wide_links[k, at : at + 8, :] for k in range(4)]
            inside, total = exchange(lambda c, where: state[before, c, where : where + 8, :], weights, at)
            effective = [total[c] + wide_field[c, at : at + 8, :] for c in range(3)]
            effective[2] = effective[2] - inside[2]
            moved = torque_of(inside, effective)
            for c in range(3):
                state[after, c, at : at + 8, :] = inside[c] + FINE * step_time * moved[c]

    def native(n):
        return state[n % 2, :, pl.ds(pl.multiple_of(top + core * strip, 8), strip), :]

    def step_pair(n, carry):
        coarse_step(0)
        coarse_step(1)
        return carry

    lax.fori_loop(0, axis_x, step_pair, 0)
    def send_start():
        for copy in start_swaps:
            copy.start()

    @pl.when(zh == 1)
    def _():
        theirs[...] = native(0)
        send_start()

    @pl.when(zh == 0)
    def _():
        base[0] = native(0)

    coarse_step(0)

    @pl.when(zh == 0)
    def _():
        theirs[...] = native(1)
        send_start()

    @pl.when(zh == 1)
    def _():
        base[0] = native(1)

    def fill(i, carry):
        at = pl.multiple_of(i * 64, 64)
        slot_rows = at + lax.broadcasted_iota(jnp.int32, (64, width), 0)
        slot_columns = share * width + lax.broadcasted_iota(jnp.int32, (64, width), 1)
        unit_length = 2.0 * math.pi / (2 * grid)

        def parts(odd_rows, odd_columns):
            rows = jnp.where((slot_rows == 0) & (odd_rows == 1), grid, slot_rows)
            columns = jnp.where((slot_columns == 0) & (odd_columns == 1), grid, slot_columns)
            wave_rows = unit_length * rows.astype(jnp.float32)
            wave_columns = unit_length * columns.astype(jnp.float32)
            squared = wave_rows * wave_rows + wave_columns * wave_columns
            nonzero = squared > 0.0
            safe = jnp.where(nonzero, squared, 1.0)
            scaled = jnp.sqrt(safe) * thickness
            film = jnp.where(nonzero, (1.0 - jnp.exp(-scaled)) / scaled, 1.0)
            weight = jnp.where(slot_rows == 0, 1.0, 2.0) * jnp.where(slot_columns == 0, 1.0, 2.0)
            weight = weight * (-1.0 / (4 * grid * grid))
            return wave_rows, wave_columns, film, (1.0 - film) / safe, weight

        @pl.when(core == 1)
        def _():
            wave_rows, wave_columns, _, in_plane, weight = parts(row_odd, column_odd)
            tensors[0, pl.ds(at, 64), :] = in_plane * wave_columns * wave_columns * weight
            mixed = in_plane * wave_columns * wave_rows * weight
            sign = jnp.where((row_odd == column_odd) == (zh == 0), -1.0, 1.0)
            tensors[2, pl.ds(at, 64), :] = jnp.where((slot_rows == 0) | (slot_columns == 0), 0.0, mixed * sign)
            wave_rows, wave_columns, _, in_plane, weight = parts(1 - row_odd, 1 - column_odd)
            tensors[1, pl.ds(at, 64), :] = in_plane * wave_rows * wave_rows * weight

        @pl.when(core == 0)
        def _():
            _, _, film, _, weight = parts(row_odd, column_odd)
            tensors[0, pl.ds(at, 64), :] = film * weight

        return carry

    lax.fori_loop(0, grid // 64, fill, 0)

    for load in loads[3:]:
        load.wait()
    for k in range(4):
        links[0, k] = wide_links[k, pl.ds(pl.multiple_of(top + core * strip, 8), strip), :]
    current[0, :, 8 : 8 + strip, :] = base[0]
    probe[0] = base[0]

    own_lines = pl.ds(pl.multiple_of(number * strip, strip), strip)

    def across(r):
        return (rest // 2 + r // 2) % (rest_count // 2) * 2 + (rest + r) % 2

    def to_unit(plane, r):
        kind, slot = (1, plane) if plane < 2 else (0, 0)
        target = across(r)
        return remote(
            send.at[plane, target // multi], land.at[slot, own_lines, :],
            send_sems.at[plane, r], land_sems.at[slot, number], at_place(kind, target),
        )

    def landed(slot, index):
        return remote(
            send.at[slot, 0], land.at[slot, pl.ds(index * strip, strip), :],
            send_sems.at[slot, 0], land_sems.at[slot, index], owner(index),
        )

    def to_owner(plane, k):
        slot = plane if plane < 2 else 0
        target = across(k // 2)
        spot = jnp.where(zh == 0, target, rest_count - 1 - target)
        index = 2 * spot + (core + k) % 2
        return remote(
            back.at[slot, pl.ds(index * strip, strip), :], got.at[plane, rest],
            back_sems.at[slot, k], got_sems.at[plane, rest], owner(index),
        )

    def gotten(plane, r):
        kind, slot = (1, plane) if plane < 2 else (0, 0)
        return remote(
            back.at[slot, pl.ds(0, strip), :], got.at[plane, r],
            back_sems.at[slot, 0], got_sems.at[plane, r], at_place(kind, r),
        )

    def each(first, last, action):
        def one(k, carry):
            action(k)
            return carry

        lax.fori_loop(first, last, one, 0)

    def push(plane):
        each(0, space - 1, lambda k: to_owner(plane, space - 1 - k).start())
        got[plane, rest] = back[plane if plane < 2 else 0, own_lines, :]

    def transform(kind, passes):
        planes = [(row_odd, column_odd), (1 - row_odd, 1 - column_odd)] if kind == 1 else [(row_odd, column_odd)]
        columns = pl.ds(pl.multiple_of(share * width, width), width)
        for n, (_, odd) in enumerate(planes):
            each(1, space, lambda k: landed(n, (number + k) % space).wait_recv())
            spectrum = product(
                passes, split(land[n]), (table_high[odd, :, columns], table_low[odd, :, columns])
            )
            put(passes, (plane_high, plane_low), n, spectrum)
        step = half

        def mix(i, carry):
            at = pl.multiple_of(i * step, step)
            lines = pl.ds(at, step)
            both = [
                product(
                    passes, (turned_high[odd, lines, :], turned_low[odd, lines, :]), (plane_high[n], plane_low[n])
                )
                for n, (odd, _) in enumerate(planes)
            ]
            if kind == 1:
                cross_term = tensors[2, lines, :]
                values = [
                    tensors[0, lines, :] * both[0] + cross_term * both[1],
                    cross_term * both[0] + tensors[1, lines, :] * both[1],
                ]
            else:
                values = [tensors[0, lines, :] * both[0]]
            for n, value in enumerate(values):
                put(passes, (mixed_high, mixed_low), (n, lines), value)
            return carry

        lax.fori_loop(0, grid // step, mix, 0)
        for n, (odd_rows, odd_columns) in enumerate(planes):
            film = product(
                passes, (table_high[odd_rows], table_low[odd_rows]), (mixed_high[n], mixed_low[n])
            )
            back[n] = product(
                passes, split(film), (turned_high[odd_columns, columns, :], turned_low[odd_columns, columns, :])
            )
            push(n if kind == 1 else 2)

    def unit_work(kind, passes):
        @pl.when(core == kind)
        def _():
            transform(kind, passes)

    def unit_end(kind):
        @pl.when(core == kind)
        def _():
            for plane in (0, 1) if kind == 1 else (2,):
                each(1, space, lambda k: to_owner(plane, k).wait_send())

    def elsewhere(plane, r, action):
        pl.when((core != (1 if plane < 2 else 0)) | (r != 0))(action)

    def evaluate(parity, passes, first, last_one=None):
        outward = remote(
            edge_out.at[0], edge_in.at[parity, 1], edge_sems.at[parity, 0], edge_sems.at[parity, 1],
            owner((number + space - 1) % space),
        )
        inward = remote(
            edge_out.at[1], edge_in.at[parity, 0], edge_sems.at[parity, 2], edge_sems.at[parity, 3],
            owner((number + 1) % space),
        )
        fold_passes = min(passes, 2)
        for c in range(3):
            if first:
                start_swaps[c].wait()
                base[1, c] = far_start[c]
                probe[1, c] = far_start[c]
                current[1, c, 8 : 8 + strip, :] = far_start[c]
            near, far = probe[0, c], probe[1, c]
            lines = pl.ds(2 * c * strip, 2 * strip)
            for p, value in enumerate((near + far, near - far)):
                put(fold_passes, (wide_high, wide_low), pl.ds((2 * c + p) * strip, strip), value)
            folded = product(fold_passes, (wide_high[lines, :], wide_low[lines, :]), (fold[...],))
            for p in range(2):
                for q in range(2):
                    which = 2 * (1 - p) + 1 - q if c == 1 else 2 * p + q
                    send[c, which] = folded[p * strip : (p + 1) * strip, q * half : (q + 1) * half]
            each(0, rest_count, lambda r: elsewhere(
                c, rest_count - 1 - r, lambda: to_unit(c, rest_count - 1 - r).start()
            ))

            @pl.when(core == (1 if c < 2 else 0))
            def _():
                land[c if c < 2 else 0, own_lines, :] = send[c, unit]

        for t in range(2):
            for c in range(3):
                edge_out[0, 3 * t + c : 3 * t + c + 1, :] = current[t, c, 8:9, :]
                edge_out[1, 3 * t + c : 3 * t + c + 1, :] = current[t, c, 7 + strip : 8 + strip, :]
        outward.start()
        inward.start()
        if first:
            for copy in field_swaps[EARLY:]:
                copy.start()
            coupling_swap.start()
        unit_work(1, passes)
        unit_work(0, passes)
        for c in (2, 0, 1):
            each(0, rest_count, lambda r: elsewhere(c, r, lambda: gotten(c, (rest + r) % rest_count).wait_recv()))
            lines = pl.ds(2 * c * strip, 2 * strip)
            for p in range(2):
                for q in range(2):
                    source = 2 * (1 - p) + 1 - q if c == 1 else 2 * p + q
                    value = None
                    for k in range(multi):
                        piece = got[c, source * multi + k]
                        value = piece if value is None else value + piece
                    where = (pl.ds((2 * c + p) * strip, strip), pl.ds(q * half, half))
                    put(fold_passes, (wide_high, wide_low), where, value)
            unfolded = product(fold_passes, (wide_high[lines, :], wide_low[lines, :]), (unfold[...],))
            even, odd = unfolded[:strip], unfolded[strip:]
            for t, value in enumerate((even + odd, even - odd)):
                if first:
                    demag[0, t, c] = value
                    demag[1, t, c] = value
                elif parity == 0:
                    moved = demag[0, t, c] + value
                    demag[0, t, c] = moved
                    demag[1, t, c] = moved
                else:
                    demag[1, t, c] = demag[0, t, c] + value
        outward.wait()
        inward.wait()
        if first:
            for copy in [*field_swaps, coupling_swap]:
                copy.wait()
            make_links(far_links, HALO, HALO + strip, far_coupling)
            links[1] = far_links[:, HALO : HALO + strip, :]
        last = number == space - 1
        for t in range(2):
            for c in range(3):
                current[t, c, 7:8, :] = edge_in[parity, 0, 3 * t + c : 3 * t + c + 1, :]
                facing = current[1 - t, c, 7 + strip : 8 + strip, :]
                arrived = edge_in[parity, 1, 3 * t + c : 3 * t + c + 1, :]
                current[t, c, 8 + strip : 9 + strip, :] = jnp.where(last, facing, arrived)
        for t in (1, 0):
            applied = (wide_field.at[:, pl.ds(pl.multiple_of(top + core * strip, 8), strip), :], far_field)[t]
            for at in range(0, strip, 8):
                rows_here = slice(at, at + 8)
                weights = [links[t, n, rows_here, :] for n in range(4)]
                inside, total = exchange(lambda c, where: current[t, c, where : where + 8, :], weights, 8 + at)
                effective = [total[c] + demag[1, t, c, rows_here, :] + applied[c, rows_here, :] for c in range(3)]
                moved = torque_of(inside, effective)
                for c in range(3):
                    if parity == 0:
                        rate[t, c, rows_here, :] = moved[c]
                        probe[t, c, rows_here, :] = step_time * moved[c]
                    else:
                        change = 0.5 * step_time * (rate[t, c, rows_here, :] + moved[c])
                        probe[t, c, rows_here, :] = change
                        base[t, c, rows_here, :] = base[t, c, rows_here, :] + change
            if t == 1 and last_one is not None:
                last_one()
        if parity == 0:
            current[:, :, 8 : 8 + strip, :] = base[...] + probe[...]
        else:
            current[:, :, 8 : 8 + strip, :] = base[...]
        for c in range(3):
            each(0, rest_count, lambda r: elsewhere(c, r, lambda: to_unit(c, r).wait_send()))
        unit_end(1)
        unit_end(0)

    evaluate(0, 3, True)

    def fine_step(i, carry):
        evaluate(1, PASSES, False)
        evaluate(0, PASSES, False)
        return carry

    lax.fori_loop(1, FINE, fine_step, 0)
    direct = core == zh
    away = {"core": zh, "zh": 1 - zh, "rest": mirror}
    beside = {"core": 1 - core}

    def carry_jump(t, where):
        return remote(base.at[t], jumps_in.at[core], jump_sends.at[t], jump_recvs.at[core], where)

    def await_jump(part):
        remote(base.at[0], jumps_in.at[part], jump_sends.at[0], jump_recvs.at[part], away).wait_recv()

    far, near = carry_jump(1, away), carry_jump(0, beside)
    evaluate(1, PASSES, False, far.start)

    @pl.when(jnp.logical_not(direct))
    def _():
        near.start()

    @pl.when(core == 0)
    def _():
        coarse_end[...] = state[1, :, top : top + rows, :]

    @pl.when(core == 1)
    def _():
        coarse_step(1)
        coarse_end[...] = state[0, :, top : top + rows, :]

    @pl.when(jnp.logical_not(direct))
    def _():
        await_jump(0)
        await_jump(1)

    @pl.when(direct)
    def _():
        jumps_in[core] = base[0]
        await_jump(1 - core)

    outer = jnp.where(first_block, 0, 1)
    inner = jnp.where(last_block, 1, 0)
    outgoing = [
        remote(source, target, chain_sends.at[n], chain_recvs.at[sem], in_slice(slice_number + 1, where))
        for n, (source, target, sem, where) in enumerate((
            (out, arrived.at[:, pl.ds(8, rows), :], 2, place),
            (last_out.at[0], last_in.at[outer], outer, outward_place),
            (last_out.at[1], last_in.at[inner], inner, inward_place),
        ))
    ]
    arrivals = [
        remote(source, target, chain_sends.at[0], chain_recvs.at[sem], in_slice(slice_number - 1, place))
        for source, target, sem in (
            (out, arrived.at[:, pl.ds(8, rows), :], 2),
            (last_out.at[0], last_in.at[0], 0),
            (last_out.at[1], last_in.at[1], 1),
        )
    ]

    def send_edges():
        @pl.when(later)
        def _():
            for c in range(3):
                last_out[0, c : c + 1, :] = out[c, 0:1, :]
                last_out[1, c : c + 1, :] = out[c, rows - 1 : rows, :]
            outgoing[1].start()
            outgoing[2].start()

    @pl.when(slice_number == 0)
    def _():
        for c in range(3):
            for k in range(2):
                out[c, k * strip : (k + 1) * strip, :] = jumps_in[k, c]
        send_edges()

    @pl.when(earlier)
    def _():
        for copy in arrivals:
            copy.wait_recv()
        for c in range(3):
            arrived[c, 7:8, :] = last_in[0, c : c + 1, :]
            arrived[c, 8 + rows : 9 + rows, :] = last_in[1, c : c + 1, :]

        def advance(at):
            weights = [wide_links[n, top + at : top + at + 8, :] for n in range(4)]
            inside, total = exchange(lambda c, where: arrived[c, where : where + 8, :], weights, 8 + at)
            effective = [total[c] + wide_field[c, top + at : top + at + 8, :] for c in range(3)]
            effective[2] = effective[2] - inside[2]
            moved = torque_of(inside, effective)
            k, within = at // strip, at % strip
            for c in range(3):
                jump = jumps_in[k, c, within : within + 8, :] - coarse_end[c, at : at + 8, :]
                out[c, at : at + 8, :] = inside[c] + FINE * step_time * moved[c] + jump

        advance(0)
        advance(rows - 8)
        send_edges()
        for at in range(8, rows - 8, 8):
            advance(at)

    @pl.when(later)
    def _():
        outgoing[0].start()
        for copy in outgoing:
            copy.wait_send()

    far.wait_send()

    @pl.when(jnp.logical_not(direct))
    def _():
        near.wait_send()

    @pl.when(jnp.logical_not(first_block))
    def _():
        to_outward.wait_send()

    to_inward.wait_send()

    @pl.when(zh == 1)
    def _():
        for c in range(3):
            for t in range(tiles // 2):
                low, high = slice(8 * t, 8 * t + 8), slice(rows - 8 - 8 * t, rows - 8 * t)
                upper, lower = flipped(out[c, high, :]), flipped(out[c, low, :])
                out[c, low, :] = upper
                out[c, high, :] = lower


def parareal(space, tm, start, field, coupling, tables):
    _, rows, grid = start.shape
    strip = rows // 2
    half = grid // 2
    rest_count = space // 2
    width = grid * 4 // rest_count
    f32, bf16 = jnp.float32, jnp.bfloat16
    operands = [start, field, coupling, *tables]
    return pl.pallas_call(
        functools.partial(parareal_kernel, space, tm),
        out_shape=jax.ShapeDtypeStruct((3, rows, grid), f32),
        in_specs=[pl.BlockSpec(memory_space=pl.ANY)] * TABLES,
        out_specs=pl.BlockSpec(memory_space=pltpu.VMEM),
        scratch_shapes=[
            *(pltpu.VMEM(operand.shape, operand.dtype) for operand in operands),
            pltpu.SemaphoreType.DMA((TABLES,)),
            pltpu.VMEM((2, 3, rows + 4 * HALO, grid), f32),
            pltpu.VMEM((3, rows + 4 * HALO, grid), f32),
            pltpu.VMEM((rows + 4 * HALO, grid), f32),
            pltpu.VMEM((4, rows + 4 * HALO, grid), f32),
            pltpu.VMEM((2, -(-7 * tm // 8) * 8, grid), f32),
            pltpu.VMEM((2, -(-7 * tm // 8) * 8, grid), f32),
            pltpu.VMEM((3, strip, grid), f32),
            pltpu.VMEM((3, rows, grid), f32),
            pltpu.VMEM((2, 3, strip + 16, grid), f32),
            pltpu.VMEM((2, 3, strip, grid), f32),
            pltpu.VMEM((2, 3, strip, grid), f32),
            pltpu.VMEM((2, 3, strip, grid), f32),
            pltpu.VMEM((2, 2, 3, strip, grid), f32),
            pltpu.VMEM((3, strip, grid), f32),
            pltpu.VMEM((3, strip, grid), f32),
            pltpu.VMEM((strip + 16, grid), f32),
            pltpu.VMEM((2, 4, strip, grid), f32),
            pltpu.VMEM((4, strip + 16, grid), f32),
            pltpu.VMEM((3, grid, width), f32),
            pltpu.VMEM((2, 8, grid), f32),
            pltpu.VMEM((2, 2, 8, grid), f32),
            pltpu.VMEM((6 * strip, grid), bf16),
            pltpu.VMEM((6 * strip, grid), bf16),
            pltpu.VMEM((3, 4, strip, half), f32),
            pltpu.VMEM((2, half, half), f32),
            pltpu.VMEM((2, half, half), f32),
            pltpu.VMEM((3, rest_count, strip, half), f32),
            pltpu.VMEM((2, half, width), bf16),
            pltpu.VMEM((2, half, width), bf16),
            pltpu.VMEM((2, grid, width), bf16),
            pltpu.VMEM((2, grid, width), bf16),
            pltpu.VMEM((2, 3, strip, grid), f32),
            pltpu.VMEM((3, rows + 16, grid), f32),
            pltpu.VMEM((2, 8, grid), f32),
            pltpu.VMEM((2, 8, grid), f32),
            pltpu.SemaphoreType.DMA((2, 2)),
            pltpu.SemaphoreType.DMA((2, 7)),
            pltpu.SemaphoreType.DMA((2, 4)),
            pltpu.SemaphoreType.DMA((3, rest_count)),
            pltpu.SemaphoreType.DMA((2, space)),
            pltpu.SemaphoreType.DMA((2, space)),
            pltpu.SemaphoreType.DMA((3, rest_count)),
            pltpu.SemaphoreType.DMA((2,)),
            pltpu.SemaphoreType.DMA((2,)),
            pltpu.SemaphoreType.DMA((3,)),
            pltpu.SemaphoreType.DMA((3,)),
        ],
        compiler_params=pltpu.CompilerParams(
            collective_id=0, has_side_effects=True, vmem_limit_bytes=VMEM_LIMIT
        ),
    )(*operands)


def make_shards(tm, space):
    def shards(initial_state, applied_field, coupling):
        grid = initial_state.shape[2]
        table, fold = sector_tables(grid)
        start = jnp.transpose(initial_state, (1, 0, 2))
        field = jnp.transpose(applied_field, (1, 0, 2))
        tables = [*halves(table), *halves(np.ascontiguousarray(np.transpose(table, (0, 2, 1))))]
        tables += [fold.astype(jnp.bfloat16), np.ascontiguousarray(fold.T).astype(jnp.bfloat16)]
        end = parareal(space, tm, start, field, coupling, tables)
        return jnp.transpose(end, (1, 0, 2))[None]

    return shards


def solution(mesh):
    tm, space = mesh.shape["tm"], mesh.shape["space"]
    finer = Mesh(mesh.devices.reshape(tm // 2, 2, 2, space // 2), EVERY)
    rows = ("zh", "rest")
    return jax.shard_map(
        make_shards(tm, space),
        mesh=finer,
        in_specs=(P(rows, None, None), P(rows, None, None), P(rows, None)),
        out_specs=P(("x", "core"), rows, None, None),
        check_vma=False,
    )
```
